32 devices in a mesh: dp: 2 (over x), tp: 16 (over z, y, core).
Axes of the slice: x: 2, y: 2, z: 4, core: 2. Of those that a mesh axis runs over, the one named last changes fastest.
Arguments:
- hidden: bfloat16 [2, 2048, 4096], P('dp'), parts along dimension 0
- grad_out: bfloat16 [2, 2048, 4096], P('dp'), parts along dimension 0
- norm_gain: bfloat16 [4096], replicated
- w_query: bfloat16 [4096, 4096], P(None, 'tp')
- w_key: bfloat16 [4096, 1024], replicated
- w_value: bfloat16 [4096, 1024], replicated
- w_out: bfloat16 [4096, 4096], P('tp')
Outputs:
- output 1: bfloat16 [2, 2048, 4096], P('dp'), parts along dimension 0
- output 2: bfloat16 [2, 2048, 4096], P('dp'), parts along dimension 0
- output 3: float32 [8192], P('dp'), parts along dimension 0
- output 4: float32 [8192, 4096], P('dp', 'tp'), parts along dimension 0
- output 5: float32 [8192, 2048], P('dp', 'tp'), parts along dimension 0
- output 6: float32 [8192, 2048], P('dp', 'tp'), parts along dimension 0
- output 7: float32 [8192, 4096], P(('dp', 'tp')), parts along dimension 0
There are 2 independent parts. The reference program is written for one: setup_inputs(seed, part) draws one part's arguments, and reference() takes and returns one part's arrays. A program takes and returns all parts, laid end to end along the dimension named above; an argument that names none is the same for every part.
All inputs are finite; a program needn't handle non-finite values.
Results may differ from the reference program's by a relative error of at most 0.00980688.
Values sent between devices are 32-bit elements.
A program may use at most 1 GiB of HBM per device.

```python
import math
import jax
import jax.numpy as jnp
from jax import lax

BATCH_SIZE = 1
SEQ_LEN = 2048
D_MODEL = 4096
Q_HEADS = 32
KV_HEADS = 8
HEAD_DIM = 128
TP_SIZE = 16
NORM_EPS = 1.0e-5
ROPE_BASE = 10000.0
MASK_VALUE = -1.0e30


def setup_inputs(seed: int = 0, part: int = 0) -> dict:
    root_key = jax.random.key(seed)
    shared_key, local_key = jax.random.split(root_key)
    part_key = jax.random.fold_in(local_key, part)
    key_hidden, key_grad = jax.random.split(part_key)
    key_gain, key_query, key_key, key_value, key_out = jax.random.split(shared_key, 5)
    inner_width = Q_HEADS * HEAD_DIM
    kv_width = KV_HEADS * HEAD_DIM
    score_gain = math.sqrt(0.5 * math.log(SEQ_LEN))
    act_shape = (BATCH_SIZE, SEQ_LEN, D_MODEL)
    hidden = jax.random.normal(key_hidden, act_shape, jnp.float32)
    grad_out = jax.random.normal(key_grad, act_shape, jnp.float32)
    norm_gain = 1.0 + 0.3 * jax.random.normal(key_gain, (D_MODEL,), jnp.float32)
    w_query = jax.random.normal(key_query, (D_MODEL, inner_width), jnp.float32) * (score_gain / math.sqrt(D_MODEL))
    w_key = jax.random.normal(key_key, (D_MODEL, kv_width), jnp.float32) / math.sqrt(D_MODEL)
    w_value = jax.random.normal(key_value, (D_MODEL, kv_width), jnp.float32) / math.sqrt(D_MODEL)
    w_out = jax.random.normal(key_out, (inner_width, D_MODEL), jnp.float32) * (3.0 / math.sqrt(inner_width))
    return {
        'hidden': hidden.astype(jnp.bfloat16),
        'grad_out': grad_out.astype(jnp.bfloat16),
        'norm_gain': norm_gain.astype(jnp.bfloat16),
        'w_query': w_query.astype(jnp.bfloat16),
        'w_key': w_key.astype(jnp.bfloat16),
        'w_value': w_value.astype(jnp.bfloat16),
        'w_out': w_out.astype(jnp.bfloat16),
    }


def to_bf16(tensor):
    return tensor + lax.stop_gradient(tensor.astype(jnp.bfloat16).astype(tensor.dtype) - tensor)


def rope_tables():
    positions = jnp.arange(SEQ_LEN, dtype=jnp.float32)
    inv_freq = ROPE_BASE ** (-jnp.arange(0, HEAD_DIM, 2, dtype=jnp.float32) / HEAD_DIM)
    angles = positions[:, None] * inv_freq[None, :]
    return jnp.cos(angles), jnp.sin(angles)


def rotate_pairs(tensor, cos_t, sin_t):
    pair_view = tensor.reshape(tensor.shape[:-1] + (HEAD_DIM // 2, 2))
    even_part = pair_view[..., 0]
    odd_part = pair_view[..., 1]
    cos_b = cos_t[:, None, :]
    sin_b = sin_t[:, None, :]
    rotated = jnp.stack([even_part * cos_b - odd_part * sin_b, even_part * sin_b + odd_part * cos_b], axis=-1)
    return rotated.reshape(tensor.shape)


def group_attention(blocks):
    q_block, k_block, v_block = blocks
    scores = jnp.einsum('bqjh,bkh->bjqk', q_block, k_block) / math.sqrt(HEAD_DIM)
    causal = jnp.arange(SEQ_LEN)[:, None] >= jnp.arange(SEQ_LEN)[None, :]
    scores = jnp.where(causal, scores, MASK_VALUE)
    attn_probs = to_bf16(jax.nn.softmax(scores, axis=-1))
    return to_bf16(jnp.einsum('bjqk,bkh->bqjh', attn_probs, v_block))


def forward(hidden, norm_gain, w_query, w_key, w_value, w_out):
    heads_per_kv = Q_HEADS // KV_HEADS
    mean_sq = jnp.mean(hidden * hidden, axis=-1, keepdims=True)
    normed = to_bf16(hidden * lax.rsqrt(mean_sq + NORM_EPS) * norm_gain)
    cos_t, sin_t = rope_tables()
    q_proj = jnp.einsum('bsd,de->bse', normed, w_query).reshape(BATCH_SIZE, SEQ_LEN, Q_HEADS, HEAD_DIM)
    k_proj = jnp.einsum('bsd,de->bse', normed, w_key).reshape(BATCH_SIZE, SEQ_LEN, KV_HEADS, HEAD_DIM)
    v_proj = jnp.einsum('bsd,de->bse', normed, w_value).reshape(BATCH_SIZE, SEQ_LEN, KV_HEADS, HEAD_DIM)
    q_rot = to_bf16(rotate_pairs(q_proj, cos_t, sin_t)).reshape(BATCH_SIZE, SEQ_LEN, KV_HEADS, heads_per_kv, HEAD_DIM)
    k_rot = to_bf16(rotate_pairs(k_proj, cos_t, sin_t))
    v_heads = to_bf16(v_proj)
    attn_heads = lax.map(jax.checkpoint(group_attention), (jnp.moveaxis(q_rot, 2, 0), jnp.moveaxis(k_rot, 2, 0), jnp.moveaxis(v_heads, 2, 0)))
    attn_flat = jnp.moveaxis(attn_heads, 0, 2).reshape(BATCH_SIZE, SEQ_LEN, Q_HEADS * HEAD_DIM)
    attn_sum = jnp.einsum('bse,ed->bsd', attn_flat, w_out)
    return to_bf16(hidden + attn_sum)


def reference(hidden, grad_out, norm_gain, w_query, w_key, w_value, w_out):
    block_out, pullback = jax.vjp(forward, hidden.astype(jnp.float32), norm_gain.astype(jnp.float32), w_query.astype(jnp.float32), w_key.astype(jnp.float32), w_value.astype(jnp.float32), w_out.astype(jnp.float32))
    grad_hidden, grad_gain, grad_w_query, grad_w_key, grad_w_value, grad_w_out = pullback(grad_out.astype(jnp.float32))
    sharers = TP_SIZE // KV_HEADS
    grad_w_key_rep = jnp.repeat(grad_w_key.reshape(D_MODEL, KV_HEADS, HEAD_DIM), sharers, axis=1).reshape(D_MODEL, TP_SIZE * HEAD_DIM)
    grad_w_value_rep = jnp.repeat(grad_w_value.reshape(D_MODEL, KV_HEADS, HEAD_DIM), sharers, axis=1).reshape(D_MODEL, TP_SIZE * HEAD_DIM)
    return (block_out.astype(jnp.bfloat16), grad_hidden.astype(jnp.bfloat16), grad_gain.astype(jnp.float32), grad_w_query.astype(jnp.float32), grad_w_key_rep.astype(jnp.float32), grad_w_value_rep.astype(jnp.float32), grad_w_out.astype(jnp.float32))
```

```python
import functools
import math
import jax
import jax.numpy as jnp
from jax import lax
from jax.experimental import pallas as pl
from jax.experimental.pallas import tpu as pltpu
from jax.sharding import PartitionSpec as P

HEAD_DIM = 128
ROPE_BASE = 10000.0
MASK_VALUE = -1.0e30
SCORE_SCALE = 1.0 / math.sqrt(HEAD_DIM)

F32, BF16 = jnp.float32, jnp.bfloat16
MESH = pl.DeviceIdType.MESH
NORM_EPS = 1.0e-5
CR, CC = 8, 2048
D_MODEL = 4096
SHARD = 128
HALVES = D_MODEL // CC
PER = SHARD // CR * HALVES
R = 2 * PER
OWN, CSEND, YSEND, CONV = 4, 7, 8, 9
LAG = 3
NI = R + CONV + LAG + 1
DP, DR, D, DS = 8, 8, 16, 4


def comm_kernel(p0, p1, x_hbm, dout_hbm, gain_ref, out0, out1, gain_out,
                pbuf, upb, dnb, zb, yb, cz, cy, fb, xo, do, stage, gacc,
                psem, up_r, dn_r, z_r, y_r, cz_r, cy_r,
                up_s, dn_s, zu_s, zd_s, y_s, c_s, o_sem, l_sem):
    dp = lax.axis_index("dp")
    t = lax.axis_index("tp")
    z, y, c = t // 4, (t // 2) % 2, t % 2
    j = t % 4

    def dev(zz, yy, cc):
        return (dp, zz * 4 + yy * 2 + cc)

    def remote(src, dst, ss, rs, device):
        return pltpu.make_async_remote_copy(src_ref=src, dst_ref=dst, send_sem=ss, recv_sem=rs,
                                            device_id=device, device_id_type=MESH)

    def rowcol(r):
        kk = lax.rem(r, PER)
        return kk // HALVES, pl.multiple_of(lax.rem(kk, HALVES) * CC, CC)

    def p_copy(p, r):
        rr, cc = rowcol(r)
        return pltpu.make_async_copy(p.at[:, rr, :, pl.ds(cc, CC)], pbuf.at[lax.rem(r, DP)], psem.at[lax.rem(r, DP)])

    def p_start(r):
        @pl.when(r < PER)
        def _():
            p_copy(p0, r).start()

        @pl.when((r >= PER) & (r < R))
        def _():
            p_copy(p1, r).start()

    def up_copy(r, o, i):
        s = lax.rem(r, DR)
        return remote(upb.at[s, o], upb.at[s, o], up_s.at[o, lax.rem(i, DS)], up_r.at[o, s], dev(lax.rem(z + 1, 4), y, c))

    def up_first(r, o, i):
        s = lax.rem(r, DR)
        return remote(pbuf.at[lax.rem(r, DP), o], upb.at[s, o], up_s.at[o, lax.rem(i, DS)], up_r.at[o, s], dev(lax.rem(z + 1, 4), y, c))

    def dn_copy(r, o, i):
        s = lax.rem(r, DR)
        return remote(dnb.at[s, o], dnb.at[s, o], dn_s.at[o, lax.rem(i, DS)], dn_r.at[o, s], dev(lax.rem(z + 3, 4), y, c))

    def dn_first(r, o, i):
        s = lax.rem(r, DR)
        return remote(pbuf.at[lax.rem(r, DP), o], dnb.at[s, o], dn_s.at[o, lax.rem(i, DS)], dn_r.at[o, s], dev(lax.rem(z + 3, 4), y, c))

    def zu_copy(r, q, i):
        s = lax.rem(r, D)
        return remote(zb.at[s, q], zb.at[s, q], zu_s.at[q, lax.rem(i, DS)], z_r.at[q, s], dev(lax.rem(z + 1, 4), y, c))

    def zd_copy(r, q, i):
        s = lax.rem(r, D)
        return remote(zb.at[s, q], zb.at[s, q], zd_s.at[q, lax.rem(i, DS)], z_r.at[q, s], dev(lax.rem(z + 3, 4), y, c))

    def y_copy(r, q, i):
        s = lax.rem(r, D)
        return remote(zb.at[s, q], yb.at[s, q], y_s.at[q, lax.rem(i, DS)], y_r.at[q, s], dev(z, 1 - y, c))

    def cz_copy(r, i):
        s = lax.rem(r, D)
        return remote(zb.at[s], cz.at[s], c_s.at[0, lax.rem(i, DS)], cz_r.at[s], dev(z, y, 1 - c))

    def cy_copy(r, i):
        s = lax.rem(r, D)
        return remote(yb.at[s], cy.at[s], c_s.at[1, lax.rem(i, DS)], cy_r.at[s], dev(z, y, 1 - c))

    bufs = (zb, yb, cz, cy)

    def src_j(k):
        yy = y if k in (0, 2) else 1 - y
        cc = c if k in (0, 1) else 1 - c
        return yy * 2 + cc

    def o_copy(out, r, i, k):
        rr, cc = rowcol(r)
        b = lax.rem(i, 2)
        return pltpu.make_async_copy(stage.at[b, k], out.at[src_j(k), :, rr, :, pl.ds(cc, CC)], o_sem.at[b, k])

    def when_up(i, f):
        r = i - z
        for o in range(1, 4):
            @pl.when((r >= 0) & (r < R) & (z < o))
            def _():
                @pl.when(z == 0)
                def _():
                    f(up_first(r, o, i))

                @pl.when(z > 0)
                def _():
                    f(up_copy(r, o, i))

    def when_dn(i, f):
        r = i - 3 + z
        for o in range(0, 3):
            @pl.when((r >= 0) & (r < R) & (z > o))
            def _():
                @pl.when(z == 3)
                def _():
                    f(dn_first(r, o, i))

                @pl.when(z < 3)
                def _():
                    f(dn_copy(r, o, i))

    def when_ag(i, q, f):
        r = i - OWN - jnp.abs(z - q)
        ok = (r >= 0) & (r <= R)

        @pl.when(ok & (z >= q) & (z < 3))
        def _():
            f(zu_copy(r, q, i))

        @pl.when(ok & (z <= q) & (z > 0))
        def _():
            f(zd_copy(r, q, i))

        @pl.when(ok)
        def _():
            f(y_copy(r, q, i))

    def when_c(i, f):
        @pl.when((i - CSEND >= 0) & (i - CSEND <= R))
        def _():
            f(cz_copy(i - CSEND, i))

        @pl.when((i - YSEND >= 0) & (i - YSEND <= R))
        def _():
            f(cy_copy(i - YSEND, i))

    base = (j * 4 + z) * (SHARD // CR)
    lx = pltpu.make_async_copy(x_hbm.at[pl.ds(base, SHARD // CR)], xo, l_sem.at[0])
    ld = pltpu.make_async_copy(dout_hbm.at[pl.ds(base, SHARD // CR)], do, l_sem.at[1])
    p_start(0)
    p_start(1)
    lx.start()
    ld.start()
    gacc[...] = jnp.zeros_like(gacc)
    lx.wait()
    ld.wait()

    def body(i, _):
        ip = i - LAG

        @pl.when(ip >= 0)
        def _():
            when_up(ip, lambda cp: cp.wait_send())
            when_dn(ip, lambda cp: cp.wait_send())
            for q in range(4):
                when_ag(ip, q, lambda cp: cp.wait_send())
            when_c(ip, lambda cp: cp.wait_send())

        p_start(i + 2)

        @pl.when(i < R)
        def _():
            p_copy(p0, i).wait()

        ru = i - z
        rd = i - 3 + z

        @pl.when((ru >= 0) & (ru < R) & (z > 0))
        def _():
            for o in range(1, 4):
                @pl.when(z <= o)
                def _():
                    up_copy(ru, o, i).wait_recv()

                @pl.when(z < o)
                def _():
                    upb[lax.rem(ru, DR), o] += pbuf[lax.rem(ru, DP), o]

        @pl.when((rd >= 0) & (rd < R) & (z < 3))
        def _():
            for o in range(0, 3):
                @pl.when(z >= o)
                def _():
                    dn_copy(rd, o, i).wait_recv()

                @pl.when(z > o)
                def _():
                    dnb[lax.rem(rd, DR), o] += pbuf[lax.rem(rd, DP), o]

        rf = i - 3

        @pl.when((rf >= 0) & (rf < R))
        def _():
            fs = lax.rem(rf, 2)
            fb[fs] = pbuf[lax.rem(rf, DP), z]

            @pl.when(z > 0)
            def _():
                fb[fs] += upb[lax.rem(rf, DR), z]

            @pl.when(z < 3)
            def _():
                fb[fs] += dnb[lax.rem(rf, DR), z]

            rr, cc = rowcol(rf)

            @pl.when(rf < PER)
            def _():
                zb[lax.rem(rf, D), z] = (xo[rr, :, pl.ds(cc, CC)].astype(F32) + fb[fs]).astype(BF16).astype(F32)

            @pl.when((rf >= PER) & (fs == 1))
            def _():
                xr = xo[rr].astype(F32)
                inv = lax.rsqrt(jnp.mean(xr * xr, axis=-1, keepdims=True) + NORM_EPS)
                u = xr * inv
                dn = jnp.concatenate([fb[0], fb[1]], axis=1)
                gg = dn * gain_ref[...]
                m = jnp.mean(gg * u, axis=-1, keepdims=True)
                dx = (do[rr].astype(F32) + inv * (gg - u * m)).astype(BF16).astype(F32)
                gacc[...] += dn * u
                zb[lax.rem(rf - 1, D), z] = dx[:, :CC]
                zb[lax.rem(rf, D), z] = dx[:, CC:]

        @pl.when(rf == R)
        def _():
            zb[R % D, z] = jnp.concatenate(
                [jnp.sum(gacc[...], axis=0, keepdims=True).reshape(HALVES, CC), jnp.zeros((CR - HALVES, CC), F32)], axis=0)

        when_up(i, lambda cp: cp.start())
        when_dn(i, lambda cp: cp.start())

        for q in range(4):
            r = i - OWN - jnp.abs(z - q)

            @pl.when((r >= 0) & (r <= R) & (z != q))
            def _():
                zu_copy(r, q, i).wait_recv()

            when_ag(i, q, lambda cp: cp.start())

        @pl.when((i - YSEND >= 0) & (i - YSEND <= R))
        def _():
            for q in range(4):
                y_copy(i - YSEND, q, i).wait_recv()

        when_c(i, lambda cp: cp.start())

        io = i - 2
        ro = io - CONV
        for k in range(4):
            @pl.when((ro >= 0) & (ro < R))
            def _():
                o_copy(out0, ro, io, k).wait()

        rc = i - CONV

        @pl.when((rc >= 0) & (rc <= R))
        def _():
            cz_copy(rc, i).wait_recv()
            cy_copy(rc, i).wait_recv()

        @pl.when((rc >= 0) & (rc < R))
        def _():
            b = lax.rem(i, 2)
            s = lax.rem(rc, D)
            for k in range(4):
                for q in range(4):
                    stage[b, k, q] = bufs[k][s, q].astype(BF16)
            for k in range(4):
                @pl.when(rc < PER)
                def _():
                    o_copy(out0, rc, i, k).start()

                @pl.when(rc >= PER)
                def _():
                    o_copy(out1, rc, i, k).start()

        @pl.when(rc == R)
        def _():
            acc = jnp.zeros((CR, CC), F32)
            for k in range(4):
                for q in range(4):
                    acc = acc + bufs[k][R % D, q]
            gain_out[...] = acc
        return 0

    lax.fori_loop(0, NI, body, 0)


def comm(p0, p1, x, dout, gain):
    anyspec = pl.BlockSpec(memory_space=pl.ANY)
    vm = pl.BlockSpec(memory_space=pltpu.VMEM)
    dma = pltpu.SemaphoreType.DMA
    ch = (CR, CC)
    return pl.pallas_call(
        comm_kernel,
        out_shape=(jax.ShapeDtypeStruct((4, 4, SHARD // CR, CR, D_MODEL), BF16),
                   jax.ShapeDtypeStruct((4, 4, SHARD // CR, CR, D_MODEL), BF16),
                   jax.ShapeDtypeStruct((CR, CC), F32)),
        in_specs=[anyspec, anyspec, anyspec, anyspec, vm],
        out_specs=(anyspec, anyspec, vm),
        scratch_shapes=[
            pltpu.VMEM((DP, 4) + ch, F32), pltpu.VMEM((DR, 4) + ch, F32), pltpu.VMEM((DR, 4) + ch, F32),
            pltpu.VMEM((D, 4) + ch, F32), pltpu.VMEM((D, 4) + ch, F32), pltpu.VMEM((D, 4) + ch, F32), pltpu.VMEM((D, 4) + ch, F32),
            pltpu.VMEM((2,) + ch, F32),
            pltpu.VMEM((SHARD // CR, CR, D_MODEL), BF16), pltpu.VMEM((SHARD // CR, CR, D_MODEL), BF16),
            pltpu.VMEM((2, 4, 4) + ch, BF16), pltpu.VMEM((CR, D_MODEL), F32),
            dma((DP,)), dma((4, DR)), dma((4, DR)), dma((4, D)), dma((4, D)), dma((D,)), dma((D,)),
            dma((4, DS)), dma((4, DS)), dma((4, DS)), dma((4, DS)), dma((4, DS)), dma((2, DS)), dma((2, 4)), dma((2,)),
        ],
        compiler_params=pltpu.CompilerParams(has_side_effects=True, vmem_limit_bytes=60 * 1024 * 1024),
        name="comm",
    )(p0, p1, x, dout, gain)


def rope_tables(seq_len):
    positions = jnp.arange(seq_len, dtype=jnp.float32)
    inv_freq = ROPE_BASE ** (-jnp.arange(0, HEAD_DIM, 2, dtype=jnp.float32) / HEAD_DIM)
    angles = positions[:, None] * inv_freq[None, :]
    return jnp.cos(angles), jnp.sin(angles)


def rotate_pairs(tensor, cos_t, sin_t):
    pair_view = tensor.reshape(tensor.shape[:-1] + (HEAD_DIM // 2, 2))
    even_part = pair_view[..., 0]
    odd_part = pair_view[..., 1]
    cos_b = cos_t[:, None, :]
    sin_b = sin_t[:, None, :]
    rotated = jnp.stack([even_part * cos_b - odd_part * sin_b, even_part * sin_b + odd_part * cos_b], axis=-1)
    return rotated.reshape(tensor.shape)


def round_kernel(v_ref, o_ref):
    o_ref[...] = v_ref[...].astype(BF16)


def rounded(v):
    rows, cols = v.shape
    br = min(rows, 256)
    bc = min(cols, 1024)
    spec = pl.BlockSpec((br, bc), lambda i, k: (i, k))
    return pl.pallas_call(round_kernel, grid=(rows // br, cols // bc), in_specs=[spec], out_specs=spec,
                          out_shape=jax.ShapeDtypeStruct(v.shape, BF16), name='rounded')(v)


def solution(mesh):
    tp_size = mesh.shape['tp']
    flip = {d: [(s, s ^ d) for s in range(tp_size)] for d in (1, 2, 3)}
    swap = [(0, 1), (1, 0)]

    def block_fn(hidden, grad_out, norm_gain, w_query, w_key, w_value, w_out):
        seq_len, d_model = hidden.shape[1:]
        x, dout = hidden[0], grad_out[0]
        t = lax.axis_index('tp')
        dp = lax.axis_index('dp')
        kv_index = t // 2
        rows = seq_len // 4
        j = t % 4

        def flip_tp(v, d):
            return lax.ppermute(v, 'tp', flip[d])

        def partner_weights(w2):
            mine = lax.dynamic_index_in_dim(w2, dp, 0, keepdims=False)
            first = flip_tp(mine, 2)
            second = lax.ppermute(first, 'dp', swap)
            return first, second

        wo2 = w_out.astype(F32).reshape(2, HEAD_DIM, d_model)
        wq2 = jnp.moveaxis(w_query.astype(F32).reshape(d_model, 2, HEAD_DIM), 1, 0)
        wo_y = partner_weights(wo2)
        wq_y = partner_weights(wq2)
        wo_c = flip_tp(w_out.astype(F32), 1)
        wq_c = flip_tp(w_query.astype(F32), 1)
        wo_yc = [flip_tp(v, 1) for v in wo_y]
        wq_yc = [flip_tp(v, 1) for v in wq_y]
        wo8 = jnp.concatenate([w_out, rounded(wo_c)] + [rounded(v) for v in list(wo_y) + wo_yc], axis=0)
        kv_pair = (t // 4) * 2
        wk_own = lax.dynamic_slice_in_dim(w_key, kv_index * HEAD_DIM, HEAD_DIM, axis=1)
        wv_own = lax.dynamic_slice_in_dim(w_value, kv_index * HEAD_DIM, HEAD_DIM, axis=1)
        wk_par = lax.dynamic_slice_in_dim(w_key, (kv_index ^ 1) * HEAD_DIM, HEAD_DIM, axis=1)
        wv_par = lax.dynamic_slice_in_dim(w_value, (kv_index ^ 1) * HEAD_DIM, HEAD_DIM, axis=1)
        wq8 = jnp.concatenate([w_query, rounded(wq_c)] + [rounded(v) for v in list(wq_y) + wq_yc]
                              + [wk_own, wv_own, wk_par, wv_par], axis=1)
        w_kv = jnp.concatenate([wk_own, wv_own], axis=1)
        cos_t, sin_t = rope_tables(seq_len)

        xf = x.astype(F32)
        inv_rms = lax.rsqrt(jnp.mean(xf * xf, axis=-1, keepdims=True) + NORM_EPS)
        gain_f32 = norm_gain.astype(F32)
        normed = (xf * inv_rms * gain_f32).astype(BF16)
        q_proj = jnp.einsum('sd,de->se', normed, w_query, preferred_element_type=F32)
        q_rot = rotate_pairs(q_proj.reshape(seq_len, 2, HEAD_DIM), cos_t, sin_t).astype(BF16)
        kv_proj = jnp.einsum('sd,de->se', normed, w_kv, preferred_element_type=F32)
        k_rot = rotate_pairs(kv_proj[:, None, :HEAD_DIM], cos_t, sin_t)[:, 0, :].astype(BF16)
        v_head = kv_proj[:, HEAD_DIM:].astype(BF16)
        scores = jnp.einsum('qjh,kh->jqk', q_rot, k_rot, preferred_element_type=F32) * SCORE_SCALE
        causal = jnp.arange(seq_len)[:, None] >= jnp.arange(seq_len)[None, :]
        attn_probs = jax.nn.softmax(jnp.where(causal, scores, MASK_VALUE), axis=-1)
        probs_bf16 = attn_probs.astype(BF16)
        attn_heads = jnp.einsum('jqk,kh->qjh', probs_bf16, v_head, preferred_element_type=F32).astype(BF16)
        attn_flat = attn_heads.reshape(seq_len, 2 * HEAD_DIM)

        grad_w_out = jnp.einsum('se,sd->ed', attn_flat, dout, preferred_element_type=F32)
        grad_heads = jnp.einsum('sd,ed->se', dout, w_out, preferred_element_type=F32).astype(BF16).reshape(seq_len, 2, HEAD_DIM)
        grad_probs = jnp.einsum('qjh,kh->jqk', grad_heads, v_head, preferred_element_type=F32)
        grad_v = jnp.einsum('jqk,qjh->kh', probs_bf16, grad_heads, preferred_element_type=F32)
        row_dot = jnp.sum(attn_probs * grad_probs, axis=-1, keepdims=True)
        grad_scores = (attn_probs * (grad_probs - row_dot) * SCORE_SCALE).astype(BF16)
        grad_q_rot = jnp.einsum('jqk,kh->qjh', grad_scores, k_rot, preferred_element_type=F32)
        grad_k_rot = jnp.einsum('jqk,qjh->kh', grad_scores, q_rot, preferred_element_type=F32)
        grad_q = rotate_pairs(grad_q_rot, cos_t, -sin_t).astype(BF16).reshape(seq_len, 2 * HEAD_DIM)
        grad_k = rotate_pairs(grad_k_rot[:, None, :], cos_t, -sin_t)[:, 0, :]
        grad_kv_part = jnp.concatenate([grad_k, grad_v], axis=-1)
        grad_kv = (grad_kv_part + flip_tp(grad_kv_part, 1)).astype(BF16)
        grad_w_query = jnp.einsum('sd,se->de', normed, grad_q, preferred_element_type=F32)
        grad_w_kv = jnp.einsum('sd,se->de', normed, grad_kv, preferred_element_type=F32)

        def block(v, jj):
            return lax.dynamic_slice_in_dim(v, jj * rows, rows, axis=0)

        def heads_first(v):
            v2 = v.reshape(seq_len, 2, HEAD_DIM)
            return jnp.where(dp == 0, v2, v2[:, ::-1]).reshape(seq_len, 2 * HEAD_DIM)

        od = jnp.concatenate([attn_flat, grad_q], axis=1)
        od_first = jnp.concatenate([heads_first(attn_flat), heads_first(grad_q)], axis=1)
        od_c = flip_tp(block(od, j ^ 1).astype(F32), 1)
        od_y = flip_tp(block(od_first, j ^ 2).astype(F32), 2)
        od_yc = flip_tp(block(od_first, j ^ 3).astype(F32), 3)
        kv_y = flip_tp(block(grad_kv, j ^ 2).astype(F32), 2)
        parts = [block(od, j), rounded(od_c), rounded(od_y), rounded(od_yc)]
        e = 2 * HEAD_DIM
        o8 = jnp.concatenate([v[:, :e] for v in parts], axis=1)
        dq8 = jnp.concatenate([v[:, e:] for v in parts] + [block(grad_kv, j), rounded(kv_y)], axis=1)
        out_part = jnp.einsum('se,ed->sd', o8, wo8, preferred_element_type=F32)
        dn_part = jnp.einsum('se,de->sd', dq8, wq8, preferred_element_type=F32)

        shard = (4, SHARD // CR, CR, d_model)
        tiles = (seq_len // CR, CR, d_model)
        out, dx, gg = comm(out_part.reshape(shard), dn_part.reshape(shard), x.reshape(tiles), dout.reshape(tiles), gain_f32.reshape(1, d_model))
        return (out.reshape(1, seq_len, d_model), dx.reshape(1, seq_len, d_model), gg[:HALVES].reshape(d_model),
                grad_w_query, grad_w_kv[:, :HEAD_DIM], grad_w_kv[:, HEAD_DIM:], grad_w_out)

    act_spec = P('dp', None, None)
    return jax.shard_map(
        block_fn, mesh=mesh,
        in_specs=(act_spec, act_spec, P(None), P(None, 'tp'), P(None, None), P(None, None), P('tp', None)),
        out_specs=(act_spec, act_spec, P('dp'), P('dp', 'tp'), P('dp', 'tp'), P('dp', 'tp'), P(('dp', 'tp'), None)),
        check_vma=False)
```

```python
import functools
import math
import jax
import jax.numpy as jnp
from jax import lax
from jax.experimental import pallas as pl
from jax.experimental.pallas import tpu as pltpu
from jax.sharding import PartitionSpec as P

F32, BF16 = jnp.float32, jnp.bfloat16
MESH = pl.DeviceIdType.MESH
NORM_EPS = 1.0e-5
MIB = 2 ** 20
TWO, FOUR, SIX = range(2), range(4), range(6)
CR, CC = 8, 2048
GC = 512
D_MODEL = 4096
SHARD = 128
RCH = SHARD // CR
HALVES = D_MODEL // CC
PER = RCH * HALVES
R = 2 * PER
OWN, CSEND, YSEND, CONV = 4, 7, 8, 9
LAG = 3
NI = R + CONV + LAG + 1
DP, DR, D, DS = 8, 8, 16, 4
ROWS, HD, TC = 512, 128, 256
TILES = D_MODEL // TC
LATER = 4
UP, DOWN = (3, 2, 1), (0, 1, 2)
T_X, T_D, T_W, T_G = 9, 10, 12, 30
NT_DIMS = (((1,), (1,)), ((), ()))
TN_DIMS = (((0,), (0,)), ((), ()))


def inside(r, n):
    return (r >= 0) & (r < n)


def scaled(a, unit):
    return pl.multiple_of(a * unit, unit)


def comm_kernel(od, od5, oc, oy, oyc, wo, foca, focb, foya, foyb, foza, fozb,
                dkv, dkv_c, n_hbm, wq, wca, wcb, wya, wk, wv, x_hbm, dout_hbm, gain_ref,
                out0, out1, gain_out, gk, gv, wyb, wza, wzb,
                pbuf, upb, dnb, zb, yb, cz, cy, fb, xo, do, stage, gacc,
                la, wof, wob, ra, p0, dqo, dqr, kva, kvs, kvr, lhs, wtf, wtq, wtk, rd, p1, dkvb, nt, gst,
                psem, up_r, dn_r, z_r, y_r, c_r,
                up_s, dn_s, zu_s, zd_s, y_s, c_s, o_sem, l_sem, e_s, e_r, w_sem, wo_sem, n_sem, g_sem):
    dp = lax.axis_index("dp")
    t = lax.axis_index("tp")
    z, y, c = t // 4, (t // 2) % 2, t % 2
    j = t % 4

    def dev(zz, yy, cc):
        return (dp, zz * 4 + yy * 2 + cc)

    above, below = dev(lax.rem(z + 1, 4), y, c), dev(lax.rem(z + 3, 4), y, c)

    def remote(src, dst, ss, rs, device):
        return pltpu.make_async_remote_copy(src_ref=src, dst_ref=dst, send_sem=ss, recv_sem=rs,
                                            device_id=device, device_id_type=MESH)

    def rowcol(r):
        kk = lax.rem(r, PER)
        first = r < PER
        row = jnp.where(first, lax.rem(kk, RCH), kk // HALVES)
        half = jnp.where(first, kk // RCH, lax.rem(kk, HALVES))
        return row, scaled(half, CC)

    def p_copy(p, r):
        rr, cc = rowcol(r)
        return pltpu.make_async_copy(p.at[:, rr, :, pl.ds(cc, CC)], pbuf.at[lax.rem(r, DP)], psem.at[lax.rem(r, DP)])

    def p_start(r):
        @pl.when(r < PER)
        def _():
            p_copy(p0, r).start()

        @pl.when((r >= PER) & (r < R))
        def _():
            p_copy(p1, r).start()

    def line_copy(buf, src, r, o, i, ss, rs, device):
        s = lax.rem(r, DR)
        return remote(pbuf.at[lax.rem(r, DP), o] if src is None else src.at[s, o], buf.at[s, o], ss.at[o, lax.rem(i, DS)], rs.at[o, s], device)

    def up_copy(r, o, i, src=upb):
        return line_copy(upb, src, r, o, i, up_s, up_r, above)

    def dn_copy(r, o, i, src=dnb):
        return line_copy(dnb, src, r, o, i, dn_s, dn_r, below)

    def cut(ref, small):
        return ref.at[:, pl.ds(0, GC)] if small else ref

    def along_z(r, q, i, small, ss, device):
        v = cut(zb.at[lax.rem(r, D), q], small)
        return remote(v, v, ss.at[q, lax.rem(i, DS)], z_r.at[q, lax.rem(r, D)], device)

    def y_copy(r, q, i, small):
        s = lax.rem(r, D)
        return remote(cut(zb.at[s, q], small), cut(yb.at[s, q], small), y_s.at[q, lax.rem(i, DS)], y_r.at[q, s], dev(z, 1 - y, c))

    def c_copy(k, r, i, small):
        s = lax.rem(r, D)
        src, dst = ((zb, cz), (yb, cy))[k]
        src, dst = src.at[s], dst.at[s]
        if small:
            src, dst = src.at[:, :, pl.ds(0, GC)], dst.at[:, :, pl.ds(0, GC)]
        return remote(src, dst, c_s.at[k, lax.rem(i, DS)], c_r.at[k, s], dev(z, y, 1 - c))

    def sized(r, f):
        @pl.when(inside(r, R))
        def _():
            f(False)

        @pl.when(r == R)
        def _():
            f(True)

    bufs = (zb, yb, cz, cy)

    def src_j(k):
        yy = y if k in (0, 2) else 1 - y
        cc = c if k in (0, 1) else 1 - c
        return yy * 2 + cc

    def o_copy(out, r, i, k):
        rr, cc = rowcol(r)
        b = lax.rem(i, 2)
        return pltpu.make_async_copy(stage.at[b, k], out.at[src_j(k), :, rr, :, pl.ds(cc, CC)], o_sem.at[b, k])

    def when_line(i, hop, order, mine, make, f):
        r = i - hop
        for o in order:
            @pl.when(inside(r, R) & mine(o))
            def _():
                @pl.when(hop == 0)
                def _():
                    f(make(r, o, i, None))

                @pl.when(hop > 0)
                def _():
                    f(make(r, o, i))

    def when_sums(i, f):
        when_line(i, z, UP, lambda o: z < o, up_copy, f)
        when_line(i, 3 - z, DOWN, lambda o: z > o, dn_copy, f)

    def when_ag(i, q, f):
        r = i - OWN - jnp.abs(z - q)

        def sends(small):
            @pl.when((z >= q) & (z < 3))
            def _():
                f(along_z(r, q, i, small, zu_s, above))

            @pl.when((z <= q) & (z > 0))
            def _():
                f(along_z(r, q, i, small, zd_s, below))

            f(y_copy(r, q, i, small))

        sized(r, sends)

    def when_c(i, f):
        sized(i - CSEND, lambda small: f(c_copy(0, i - CSEND, i, small)))
        sized(i - YSEND, lambda small: f(c_copy(1, i - YSEND, i, small)))

    def head_at(p):
        return pl.ds(scaled(dp ^ p, HD), HD)

    def rows_of(jj):
        return pl.ds(scaled(jj, ROWS), ROWS)

    def wo_loads(n):
        b = lax.rem(n, 2)
        cols = pl.ds(scaled(n, TC), TC)
        cps = [(src.at[:, cols], wof.at[b, k]) for k, src in enumerate((foca, focb, foya, foyb, foza, fozb))] + [(wo.at[:, cols], wob.at[b])]
        return [pltpu.make_async_copy(a, v, wo_sem.at[b, k]) for k, (a, v) in enumerate(cps)]

    def first_tile(n):
        b = lax.rem(n, 2)
        for cp in wo_loads(n):
            cp.wait()
        for p in TWO:
            ra[p * HD:(p + 1) * HD, :] = wob[b, head_at(p), :]
        for k in SIX:
            ra[(2 + k) * HD:(3 + k) * HD, :] = wof[b, k].astype(BF16)
        tile = jnp.dot(la[...], ra[...], preferred_element_type=F32)
        p0[:, :, :, pl.ds(scaled(n, TC), TC)] = tile.reshape(4, RCH, CR, TC)

    def dq_send(d):
        return remote(od.at[pl.ds(2, 2), rows_of(j ^ d)], dqr.at[d - 1], e_s.at[d - 1], e_r.at[d - 1], (dp, t ^ d))

    exchange = [dq_send(1), dq_send(2), dq_send(3),
                remote(kvs.at[0], kvr, e_s.at[3], e_r.at[3], (dp, t ^ 2)),
                remote(wya, wyb, e_s.at[4], e_r.at[4], (1 - dp, t)),
                remote(wya, wza, e_s.at[5], e_r.at[5], (dp, t ^ 1))]
    last = remote(wyb, wzb, e_s.at[6], e_r.at[6], (dp, t ^ 1))
    own = pltpu.make_async_copy(od.at[pl.ds(2, 2), rows_of(j)], dqo, l_sem.at[2])

    def kv_loads(m):
        rows = rows_of(j ^ 2 ^ m)
        return [pltpu.make_async_copy(src.at[rows], kva.at[k], l_sem.at[3 + k]) for k, src in enumerate((dkv, dkv_c))]

    def kv_sum(m, out):
        for cp in kv_loads(m):
            cp.wait()
        total = kva[0] + kva[1]
        dkvb[rows_of(j ^ 2 ^ m), :] = total.astype(BF16)
        if out is not None:
            kvs[out] = total

    kv_own = t // 2

    def tile_loads(n):
        b = lax.rem(n, 2)
        r = pl.ds(scaled(n, TC), TC)
        cps = [(src.at[r], wtf.at[b, k]) for k, src in enumerate((wca, wcb, wya, wyb, wza, wzb))] + [(wq.at[r], wtq.at[b])]
        cps += [(src.at[r, pl.ds(scaled(h, HD), HD)], wtk.at[b, k])
                for k, (src, h) in enumerate(((wk, kv_own), (wv, kv_own), (wk, kv_own ^ 1), (wv, kv_own ^ 1)))]
        return [pltpu.make_async_copy(a, v, w_sem.at[b, k]) for k, (a, v) in enumerate(cps)]

    def second_tile(n):
        b = lax.rem(n, 2)
        for cp in tile_loads(n):
            cp.wait()
        for p in TWO:
            rd[:, p * HD:(p + 1) * HD] = wtq[b, :, head_at(p)]
        for k in SIX:
            rd[:, (2 + k) * HD:(3 + k) * HD] = wtf[b, k].astype(BF16)
        for k in FOUR:
            rd[:, (8 + k) * HD:(9 + k) * HD] = wtk[b, k]
        tile = lax.dot_general(lhs[...], rd[...], NT_DIMS, preferred_element_type=F32)
        p1[:, :, :, pl.ds(scaled(n, TC), TC)] = tile.reshape(4, RCH, CR, TC)

    def n_load(n):
        b = lax.rem(n, 2)
        return pltpu.make_async_copy(n_hbm.at[:, pl.ds(scaled(n, TC), TC)], nt.at[b], n_sem.at[b])

    def g_store(n):
        b = lax.rem(n, 2)
        r = pl.ds(scaled(n, TC), TC)
        return [pltpu.make_async_copy(gst.at[b, k], g.at[r], g_sem.at[b, k]) for k, g in enumerate((gk, gv))]

    def grad_tile(n):
        b = lax.rem(n, 2)
        n_load(n).wait()
        tile = lax.dot_general(nt[b], dkvb[...], TN_DIMS, preferred_element_type=F32)
        for k in TWO:
            gst[b, k] = tile[:, k * HD:(k + 1) * HD]
        for cp in g_store(n):
            cp.start()

    def products(i):
        for at, m, out in ((LATER, 2, 1), (LATER + 1, 1, None), (LATER + 2, 3, None)):
            @pl.when(i == at)
            def _():
                kv_sum(m, out)
                if m < 3:
                    for cp in kv_loads(5 - 2 * m if m == 2 else 3):
                        cp.start()

        n = i + TILES // 2 - LATER

        @pl.when((i >= LATER) & (n + 1 < TILES))
        def _():
            for cp in wo_loads(n + 1):
                cp.start()

        @pl.when((i >= LATER) & (n < TILES))
        def _():
            first_tile(n)

        @pl.when(i == T_X)
        def _():
            exchange[4].wait()
            last.start()

        @pl.when(i == T_D)
        def _():
            for cp in [own] + exchange[:4] + exchange[5:]:
                cp.wait()
            for p in TWO:
                lhs[:, p * HD:(p + 1) * HD] = dqo[p].astype(BF16)
                for k in range(3):
                    lhs[:, (2 * k + 2 + p) * HD:(2 * k + 3 + p) * HD] = dqr[k, p].astype(BF16)
            lhs[:, 8 * HD:10 * HD] = kvs[1].astype(BF16)
            lhs[:, 10 * HD:] = kvr[...].astype(BF16)

        @pl.when(i == T_W)
        def _():
            last.wait()

        @pl.when(inside(i - T_W, TILES))
        def _():
            for cp in tile_loads(i - T_W):
                cp.start()

        @pl.when(inside(i - T_W - 1, TILES))
        def _():
            second_tile(i - T_W - 1)

        @pl.when(inside(i - T_G, TILES))
        def _():
            n_load(i - T_G).start()

        @pl.when(inside(i - T_G - 3, TILES))
        def _():
            for cp in g_store(i - T_G - 3):
                cp.wait()

        @pl.when(inside(i - T_G - 1, TILES))
        def _():
            grad_tile(i - T_G - 1)

    for cp in exchange[:3] + exchange[4:] + [own] + kv_loads(0):
        cp.start()
    base = (j * 4 + z) * RCH
    loads = [pltpu.make_async_copy(x_hbm.at[pl.ds(base, RCH)], xo, l_sem.at[0]),
             pltpu.make_async_copy(dout_hbm.at[pl.ds(base, RCH)], do, l_sem.at[1])]
    loads += [pltpu.make_async_copy(src.at[p], p0.at[:, :, :, pl.ds((2 * k + p) * HD, HD)], l_sem.at[5 + 2 * k + p])
              for k, src in enumerate((od5.at[:, pl.ds(j * 4, 4)], oc, oy, oyc)) for p in TWO]
    for cp in loads + wo_loads(0):
        cp.start()
    gacc[...] = jnp.zeros_like(gacc)
    kv_sum(0, 0)
    for cp in kv_loads(2):
        cp.start()
    for cp in loads:
        cp.wait()
    exchange[3].start()
    for k in FOUR:
        for p in TWO:
            at = slice((2 * k + p) * HD, (2 * k + p + 1) * HD)
            la[:, at] = p0[:, :, :, at].reshape(ROWS, HD).astype(BF16)

    def first_half(n, _):
        for cp in wo_loads(n + 1):
            cp.start()
        first_tile(n)
        return 0

    lax.fori_loop(0, TILES // 2, first_half, 0)
    p_start(0)
    p_start(1)

    def body(i, _):
        products(i)

        ip = i - LAG

        @pl.when(ip >= 0)
        def _():
            when_sums(ip, lambda cp: cp.wait_send())
            for q in FOUR:
                when_ag(ip, q, lambda cp: cp.wait_send())
            when_c(ip, lambda cp: cp.wait_send())

        p_start(i + 2)

        @pl.when(i < R)
        def _():
            p_copy(p0, i).wait()

        def take(r, hop, order, make, buf, past):
            @pl.when(inside(r, R) & (hop > 0))
            def _():
                for o in order:
                    @pl.when(past(o))
                    def _():
                        make(r, o, i).wait_recv()
                        buf[lax.rem(r, DR), o] += pbuf[lax.rem(r, DP), o]

        take(i - z, z, UP, up_copy, upb, lambda o: z < o)
        take(i - 3 + z, 3 - z, DOWN, dn_copy, dnb, lambda o: z > o)

        rf = i - 3
        fs = lax.rem(rf, 2)

        @pl.when(inside(rf, R))
        def _():
            fb[fs] = pbuf[lax.rem(rf, DP), z]

            @pl.when(z > 0)
            def _():
                up_copy(rf, z, i).wait_recv()
                fb[fs] += upb[lax.rem(rf, DR), z]

            @pl.when(z < 3)
            def _():
                dn_copy(rf, z, i).wait_recv()
                fb[fs] += dnb[lax.rem(rf, DR), z]

            rr, cc = rowcol(rf)

            @pl.when(rf < PER)
            def _():
                zb[lax.rem(rf, D), z] = (xo[rr, :, pl.ds(cc, CC)].astype(F32) + fb[fs]).astype(BF16).astype(F32)

            @pl.when((rf >= PER) & (fs == 1))
            def _():
                xr = xo[rr].astype(F32)
                inv = lax.rsqrt(jnp.mean(xr * xr, axis=-1, keepdims=True) + NORM_EPS)
                u = xr * inv
                dn = jnp.concatenate([fb[0], fb[1]], axis=1)
                gg = dn * gain_ref[...]
                m = jnp.mean(gg * u, axis=-1, keepdims=True)
                dx = (do[rr].astype(F32) + inv * (gg - u * m)).astype(BF16).astype(F32)
                gacc[...] += dn * u
                zb[lax.rem(rf - 1, D), z] = dx[:, :CC]
                zb[lax.rem(rf, D), z] = dx[:, CC:]

        @pl.when(rf == R)
        def _():
            total = jnp.sum(gacc[...], axis=0, keepdims=True)
            zb[R % D, z, :, :GC] = jnp.concatenate([total[:, a * GC:(a + 1) * GC] for a in range(CR)], axis=0)

        when_sums(i, lambda cp: cp.start())

        for q in FOUR:
            r = i - OWN - jnp.abs(z - q)

            @pl.when(z != q)
            def _():
                sized(r, lambda small: along_z(r, q, i, small, zu_s, above).wait_recv())

            when_ag(i, q, lambda cp: cp.start())

        for q in FOUR:
            sized(i - YSEND, lambda small: y_copy(i - YSEND, q, i, small).wait_recv())

        when_c(i, lambda cp: cp.start())

        @pl.when(inside(i - 2 - CONV, R))
        def _():
            for k in FOUR:
                o_copy(out0, i - 2 - CONV, i, k).wait()

        rc = i - CONV

        for k in TWO:
            sized(rc, lambda small: c_copy(k, rc, i, small).wait_recv())

        @pl.when(inside(rc, R))
        def _():
            b = lax.rem(i, 2)
            s = lax.rem(rc, D)
            for k in FOUR:
                for q in FOUR:
                    stage[b, k, q] = bufs[k][s, q].astype(BF16)

            @pl.when(rc < PER)
            def _():
                for k in FOUR:
                    o_copy(out0, rc, i, k).start()

            @pl.when(rc >= PER)
            def _():
                for k in FOUR:
                    o_copy(out1, rc, i, k).start()

        @pl.when(rc == R)
        def _():
            acc = jnp.zeros((CR, GC), F32)
            for k in FOUR:
                for q in FOUR:
                    acc = acc + bufs[k][R % D, q, :, :GC]
            for h in range(CR):
                for a in range(GC // HD):
                    gain_out[h * (GC // HD) + a] = acc[h, a * HD:(a + 1) * HD]

        return 0

    lax.fori_loop(0, NI, body, 0)


def comm(od, os, wo, fos, dkv, dkv_c, n, wq, wqs, wk, wv, x, dout, gain):
    anyspec = pl.BlockSpec(memory_space=pl.ANY)
    hbm = pl.BlockSpec(memory_space=pltpu.HBM)
    vm = pl.BlockSpec(memory_space=pltpu.VMEM)
    dma, vmem, sds = pltpu.SemaphoreType.DMA, pltpu.VMEM, jax.ShapeDtypeStruct
    ch = (CR, CC)
    full = sds((4, 4, RCH, CR, D_MODEL), BF16)
    land = sds((D_MODEL, HD), F32)
    part = vmem((4, RCH, CR, D_MODEL), F32)
    owned = vmem((RCH, CR, D_MODEL), BF16)
    gathered = vmem((D, 4) + ch, F32)
    line = vmem((DR, 4) + ch, F32)
    pair = vmem((2, ROWS, 2 * HD), F32)
    return pl.pallas_call(
        comm_kernel,
        out_shape=(full, full, sds((D_MODEL // HD, HD), F32)) + (land,) * 5,
        in_specs=[hbm] * 23 + [vm],
        out_specs=(anyspec, anyspec, vm) + (hbm,) * 5,
        scratch_shapes=[
            vmem((DP, 4) + ch, F32), line, line, gathered, gathered, gathered, gathered, vmem((2,) + ch, F32),
            owned, owned, vmem((2, 4, 4) + ch, BF16), vmem((CR, D_MODEL), F32),
            vmem((ROWS, 8 * HD), BF16), vmem((2, 6, HD, TC), F32), vmem((2, 2 * HD, TC), BF16),
            vmem((8 * HD, TC), BF16), part,
            vmem((2, ROWS, HD), F32), vmem((3, 2, ROWS, HD), F32), pair, pair, vmem((ROWS, 2 * HD), F32),
            vmem((ROWS, 12 * HD), BF16), vmem((2, 6, TC, HD), F32), vmem((2, TC, 2 * HD), BF16), vmem((2, 4, TC, HD), BF16),
            vmem((TC, 12 * HD), BF16), part,
            vmem((4 * ROWS, 2 * HD), BF16), vmem((2, 4 * ROWS, TC), BF16), vmem((2, 2, TC, HD), F32),
            dma((DP,)), dma((4, DR)), dma((4, DR)), dma((4, D)), dma((4, D)), dma((2, D)),
            dma((4, DS)), dma((4, DS)), dma((4, DS)), dma((4, DS)), dma((4, DS)), dma((2, DS)), dma((2, 4)), dma((13,)),
            dma((7,)), dma((7,)), dma((2, 11)), dma((2, 7)), dma((2,)), dma((2, 2)),
        ],
        compiler_params=pltpu.CompilerParams(has_side_effects=True, vmem_limit_bytes=62 * MIB),
        cost_estimate=pl.CostEstimate(flops=13 * 10**9, bytes_accessed=10**8, transcendentals=0),
        name="comm",
    )(od, od.reshape(4, 16, RCH, CR, HD), *[o.reshape(2, 4, RCH, CR, HD) for o in os], wo, *fos, dkv, dkv_c, n, wq, *wqs, wk, wv, x, dout, gain)[:5]


HEAD_DIM = 128
ROPE_BASE = 10000.0
SCORE_SCALE = 1.0 / math.sqrt(HEAD_DIM)
SEQ = 2048
NEG = -1.0e30
TILE = 256


def mm(a, b):
    return jnp.dot(a, b, preferred_element_type=F32)


def mm_nt(a, b):
    return lax.dot_general(a, b, NT_DIMS, preferred_element_type=F32)


def widen_kernel(axis, dp_ref, w_ref, *outs):
    for p, out in enumerate(outs):
        at = pl.ds(scaled(dp_ref[0] ^ p, HEAD_DIM), HEAD_DIM)
        out[...] = (w_ref[:, at] if axis else w_ref[at, :]).astype(F32)


def widen(dp, w, axis):
    tile = 1024
    shape = lambda width: (tile, width) if axis else (width, tile)
    index = (lambda i, s: (i, 0)) if axis else (lambda i, s: (0, i))
    half = jax.ShapeDtypeStruct((D_MODEL, HEAD_DIM) if axis else (HEAD_DIM, D_MODEL), F32)
    return pl.pallas_call(
        functools.partial(widen_kernel, axis),
        grid_spec=pltpu.PrefetchScalarGridSpec(
            num_scalar_prefetch=1, grid=(D_MODEL // tile,),
            in_specs=[pl.BlockSpec(shape(2 * HEAD_DIM), index)],
            out_specs=(pl.BlockSpec(shape(HEAD_DIM), index),) * len(TWO)),
        out_shape=(half,) * len(TWO),
        cost_estimate=pl.CostEstimate(flops=10**9, bytes_accessed=6 * MIB, transcendentals=0),
        name="widen")(dp, w)


def swap_pairs(v):
    lane = lax.broadcasted_iota(jnp.int32, v.shape, 1)
    return jnp.where(lane % 2 == 0, pltpu.roll(v, HEAD_DIM - 1, 1), pltpu.roll(v, 1, 1))


def rotate(v, cos_v, sin_v):
    return v * cos_v + swap_pairs(v) * sin_v


def tile_angles(cos_ref, sin_ref, i):
    at = pl.ds(TILE + i, 1)
    ca, sa = cos_ref[at, :], sin_ref[at, :]
    cb, sb = cos_ref[:TILE, :], sin_ref[:TILE, :]
    even = lax.broadcasted_iota(jnp.int32, (TILE, HEAD_DIM), 1) % 2 == 0
    s = sa * cb + ca * sb
    return ca * cb - sa * sb, jnp.where(even, -s, s)


def proj_kernel(kv_ref, x_ref, dout_ref, gain_ref, wq_ref, wk_ref, wv_ref, wo_ref, cos_ref, sin_ref,
                n_ref, q_ref, k_ref, v_ref, do_ref, wkv):
    @pl.when(pl.program_id(0) == 0)
    def _():
        wkv[:, :HEAD_DIM] = wk_ref[...]
        wkv[:, HEAD_DIM:] = wv_ref[...]

    xf = x_ref[...].astype(F32)
    inv = lax.rsqrt(jnp.mean(xf * xf, axis=-1, keepdims=True) + NORM_EPS)
    n_ref[...] = (xf * inv * gain_ref[...]).astype(BF16)
    n = n_ref[...]
    q = mm(n, wq_ref[...])
    kv = mm(n, wkv[...])
    d = mm_nt(dout_ref[...], wo_ref[...])
    cos_v, sin_v = tile_angles(cos_ref, sin_ref, pl.program_id(0))
    for h in TWO:
        cols = slice(h * HEAD_DIM, (h + 1) * HEAD_DIM)
        q_ref[h] = rotate(q[:, cols], cos_v, sin_v).astype(BF16)
        do_ref[h] = d[:, cols].astype(BF16)
    k_ref[...] = rotate(kv[:, :HEAD_DIM], cos_v, sin_v).astype(BF16)
    v_ref[...] = kv[:, HEAD_DIM:].astype(BF16)


def proj(kv, x, dout, gain, w_query, w_key, w_value, w_out, cos_t, sin_t):
    row = lambda w: pl.BlockSpec((TILE, w), lambda i, s: (i, 0))
    whole = lambda a, b: pl.BlockSpec((a, b), lambda i, s: (0, 0))
    head2 = pl.BlockSpec((2, TILE, HEAD_DIM), lambda i, s: (0, i, 0))
    wspec = pl.BlockSpec((D_MODEL, HEAD_DIM), lambda i, s: (0, s[0]))
    sds = jax.ShapeDtypeStruct
    return pl.pallas_call(
        proj_kernel,
        grid_spec=pltpu.PrefetchScalarGridSpec(
            num_scalar_prefetch=1, grid=(SEQ // TILE,),
            in_specs=[row(D_MODEL), row(D_MODEL), whole(1, D_MODEL), whole(D_MODEL, 2 * HEAD_DIM), wspec, wspec,
                      whole(2 * HEAD_DIM, D_MODEL)] + [whole(TILE + SEQ // TILE, HEAD_DIM)] * 2,
            out_specs=(row(D_MODEL), head2, row(HEAD_DIM), row(HEAD_DIM), head2),
            scratch_shapes=[pltpu.VMEM((D_MODEL, 2 * HEAD_DIM), BF16)]),
        out_shape=(sds((SEQ, D_MODEL), BF16), sds((2, SEQ, HEAD_DIM), BF16), sds((SEQ, HEAD_DIM), BF16),
                   sds((SEQ, HEAD_DIM), BF16), sds((2, SEQ, HEAD_DIM), BF16)),
        compiler_params=pltpu.CompilerParams(vmem_limit_bytes=56 * MIB),
        cost_estimate=pl.CostEstimate(flops=2 * SEQ * D_MODEL * 768, bytes_accessed=58 * MIB, transcendentals=0),
        name="proj")(kv, x, dout, gain, w_query, w_key, w_value, w_out, cos_t, sin_t)


def attn_kernel(first, nt, dp_ref, q_ref, do_ref, k_ref, v_ref, cos_ref, sin_ref, *refs):
    prev, (o_ref, dq_ref, od_ref, dkv_ref, kt, vt, qt, dot_, qc, dc, s) = refs[:-11], refs[-11:]
    i = pl.program_id(0) + first
    wide = 2 * TILE
    c2 = SCORE_SCALE * math.log2(math.e)

    @pl.when(i == first)
    def _():
        def turn(b, _):
            r = pl.ds(pl.multiple_of(b * TILE, TILE), TILE)
            kt[b] = k_ref[r, :].T
            vt[b] = v_ref[r, :].T
            dkv_ref[r, :] = prev[-1][r, :] if prev else jnp.zeros((TILE, 2 * HEAD_DIM), F32)
            return 0

        lax.fori_loop(0, nt, turn, 0)

    for h in TWO:
        r = slice(h * TILE, (h + 1) * TILE)
        qc[r, :] = q_ref[h]
        dc[r, :] = do_ref[h]
        qt[:, r] = q_ref[h].T
        dot_[:, r] = do_ref[h].T

    def keys(b):
        return pl.ds(pl.multiple_of(b * TILE, TILE), TILE)

    def fold(f, v):
        a = v[:8]
        for g in range(1, TILE // 8):
            a = f(a, v[g * 8:(g + 1) * 8])
        return a

    def score(b, m):
        sb = mm(k_ref[keys(b), :], qt[...])
        s[b] = sb
        return jnp.maximum(m, fold(jnp.maximum, sb))

    m8 = lax.fori_loop(0, i, score, jnp.full((8, wide), NEG, F32))
    sb = mm(k_ref[keys(i), :], qt[...])
    key = lax.broadcasted_iota(jnp.int32, (TILE, wide), 0)
    query = lax.broadcasted_iota(jnp.int32, (TILE, wide), 1) % TILE
    sb = jnp.where(key <= query, sb, NEG)
    s[i] = sb
    m8 = jnp.maximum(m8, fold(jnp.maximum, sb))
    m = jnp.max(m8, axis=0, keepdims=True) * c2

    def expo(b, l):
        p = jnp.exp2(s[b] * c2 - m)
        s[b] = p
        return l + fold(jnp.add, p)

    l8 = lax.fori_loop(0, i + 1, expo, jnp.zeros((8, wide), F32))
    inv_l = 1.0 / jnp.sum(l8, axis=0, keepdims=True)

    def value(b, acc):
        p = s[b] * inv_l
        s[b] = p
        return acc + mm(vt[b], p.astype(BF16))

    ot = lax.fori_loop(0, i + 1, value, jnp.zeros((HEAD_DIM, wide), F32))
    row_dot = jnp.sum(ot * dot_[...].astype(F32), axis=0, keepdims=True)

    def grads(b, acc):
        p = s[b]
        dp = mm(v_ref[keys(b), :], dot_[...])
        ds = (p * (dp - row_dot)).astype(BF16)
        dkv_ref[keys(b), :HEAD_DIM] += mm(ds, qc[...])
        dkv_ref[keys(b), HEAD_DIM:] += mm(p.astype(BF16), dc[...])
        return acc + mm(kt[b], ds)

    dqt = lax.fori_loop(0, i + 1, grads, jnp.zeros((HEAD_DIM, wide), F32))

    cos_v, sin_v = tile_angles(cos_ref, sin_ref, i)
    for h in TWO:
        cols = slice(h * HEAD_DIM, (h + 1) * HEAD_DIM)
        r = slice(h * TILE, (h + 1) * TILE)
        o = ot[:, r].T.astype(BF16)
        dq = rotate(dqt[:, r].T * SCORE_SCALE, cos_v, -sin_v).astype(BF16)
        o_ref[:, cols] = o
        dq_ref[:, cols] = dq
        place = dp_ref[0] ^ h
        od_ref[place] = o.astype(F32)
        od_ref[2 + place] = dq.astype(F32)

    if prev:
        @pl.when(i == nt - 1)
        def _():
            def finish(b, _):
                r = keys(b)
                cos_b, sin_b = tile_angles(cos_ref, sin_ref, b)
                dkv_ref[r, :HEAD_DIM] = rotate(dkv_ref[r, :HEAD_DIM] * SCORE_SCALE, cos_b, -sin_b)
                return 0

            lax.fori_loop(0, nt, finish, 0)


def attention(dp, q, do, k, v, cos_t, sin_t, first, count, prev):
    n = SEQ // TILE
    head2 = pl.BlockSpec((2, TILE, HEAD_DIM), lambda i, s: (0, i + first, 0))
    whole = pl.BlockSpec((SEQ, HEAD_DIM), lambda i, s: (0, 0))
    angle = pl.BlockSpec((TILE + n, HEAD_DIM), lambda i, s: (0, 0))
    both = pl.BlockSpec((TILE, 2 * HEAD_DIM), lambda i, s: (i + first, 0))
    sums = pl.BlockSpec((SEQ, 2 * HEAD_DIM), lambda i, s: (0, 0))
    sds, vmem = jax.ShapeDtypeStruct, pltpu.VMEM
    heads_t, turned, stacked = vmem((n, HEAD_DIM, TILE), BF16), vmem((HEAD_DIM, 2 * TILE), BF16), vmem((2 * TILE, HEAD_DIM), BF16)
    args = (dp, q, do, k, v, cos_t, sin_t)
    return pl.pallas_call(
        functools.partial(attn_kernel, first, n),
        grid_spec=pltpu.PrefetchScalarGridSpec(
            num_scalar_prefetch=1, grid=(count,),
            in_specs=[head2, head2, whole, whole, angle, angle] + ([pl.BlockSpec(memory_space=pl.ANY)] * 3 + [sums] if prev else []),
            out_specs=(both, both, pl.BlockSpec((4, TILE, HEAD_DIM), lambda i, s: (0, i + first, 0)), sums),
            scratch_shapes=[heads_t, heads_t, turned, turned, stacked, stacked, vmem((n, TILE, 2 * TILE), F32)]),
        out_shape=(sds((SEQ, 2 * HEAD_DIM), BF16), sds((SEQ, 2 * HEAD_DIM), BF16), sds((4, SEQ, HEAD_DIM), F32), sds((SEQ, 2 * HEAD_DIM), F32)),
        input_output_aliases={len(args) + a: a for a in range(len(prev))},
        compiler_params=pltpu.CompilerParams(vmem_limit_bytes=56 * MIB),
        cost_estimate=pl.CostEstimate(flops=6 * 10**9, bytes_accessed=14 * MIB, transcendentals=10**6),
        name="attention")(*args, *prev)


def rope_tables():
    lane = jnp.arange(HEAD_DIM)
    inv_freq = ROPE_BASE ** (-(lane - lane % 2).astype(F32) / HEAD_DIM)
    rows = jnp.concatenate([jnp.arange(TILE), jnp.arange(SEQ // TILE) * TILE]).astype(F32)
    angles = rows[:, None] * inv_freq[None, :]
    return jnp.cos(angles), jnp.sin(angles)


def block_fn(hidden, grad_out, norm_gain, w_query, w_key, w_value, w_out):
    seq_len, d_model = hidden.shape[1:]
    x, dout = hidden[0], grad_out[0]
    t = lax.axis_index('tp')
    dp = lax.axis_index('dp')
    j = t % 4
    rows = seq_len // 4
    pre = jnp.stack([dp, j, t // 2]).astype(jnp.int32)
    dpa, kva = pre[0:1], pre[2:3]

    def flip(v, d):
        return lax.ppermute(v, 'tp', [(s, s ^ d) for s in range(16)])

    def over_x(v):
        return lax.ppermute(v, 'dp', [(0, 1), (1, 0)])

    woa, wob = widen(dpa, w_out, 0)
    wo_ya = flip(woa, 2)
    wo_yb = over_x(wo_ya)
    fos = [flip(woa, 1), flip(wob, 1), wo_ya, wo_yb, flip(wo_ya, 1), flip(wo_yb, 1)]
    kva, w_query_, _ = lax.optimization_barrier((kva, w_query, woa))
    cos_t, sin_t = rope_tables()
    gain = norm_gain.astype(F32).reshape(1, d_model)
    n, q, k, v, do = proj(kva, x, dout, gain, w_query_, w_key, w_value, w_out, cos_t, sin_t)
    dpb, _ = lax.optimization_barrier((dpa, k))
    wqa, wqb = widen(dpb, w_query, 1)
    wqs = [flip(wqa, 1), flip(wqb, 1), flip(wqa, 2)]
    dpc, _ = lax.optimization_barrier((dpa, wqa))
    part = attention(dpc, q, do, k, v, cos_t, sin_t, 0, SEQ // TILE // 2, ())
    o, dq, od, dkv_part = attention(dpc, q, do, k, v, cos_t, sin_t, SEQ // TILE // 2, SEQ // TILE // 2, part)

    def rows_of(jj):
        return lax.dynamic_slice(od, (0, jj * rows, 0), (2, rows, HEAD_DIM))

    os = [flip(rows_of(j ^ d), d) for d in (1, 2, 3)]
    dkv_c = flip(dkv_part, 1)
    grad_w_query = jnp.einsum('sd,se->de', n, dq, preferred_element_type=F32)
    grad_w_out = jnp.einsum('se,sd->ed', o, dout, preferred_element_type=F32)

    tiles = (seq_len // CR, CR, d_model)
    out, dx, gg, gk, gv = comm(od, os, w_out, fos, dkv_part, dkv_c, n, w_query, wqs, w_key, w_value,
                               x.reshape(tiles), dout.reshape(tiles), gain)
    return (out.reshape(1, seq_len, d_model), dx.reshape(1, seq_len, d_model), gg.reshape(d_model), grad_w_query, gk, gv, grad_w_out)


def solution(mesh):
    act_spec = P('dp', None, None)

    return jax.shard_map(
        block_fn, mesh=mesh,
        in_specs=(act_spec, act_spec, P(None), P(None, 'tp'), P(None, None), P(None, None), P('tp', None)),
        out_specs=(act_spec, act_spec, P('dp'), P('dp', 'tp'), P('dp', 'tp'), P('dp', 'tp'), P(('dp', 'tp'), None)),
        check_vma=False)
```

```python
import functools
import math
import jax
import jax.numpy as jnp
from jax import lax
from jax.experimental import pallas as pl
from jax.experimental.pallas import tpu as pltpu
from jax.sharding import PartitionSpec as P

F32, BF16 = jnp.float32, jnp.bfloat16
MESH = pl.DeviceIdType.MESH
NORM_EPS = 1.0e-5
MIB = 2 ** 20
TWO, FOUR, SIX = range(2), range(4), range(6)
CR, CC = 8, 2048
GC = 512
D_MODEL = 4096
SHARD = 128
RCH = SHARD // CR
HALVES = D_MODEL // CC
PER = RCH * HALVES
R = 2 * PER
OWN, CSEND, YSEND, CONV = 4, 7, 8, 9
LAG = 3
L, QUICK = R - 1, 2
NI = R + CONV + 1
DP, DR, D, DS = 8, 8, 16, 4
ROWS, HD, TC = 512, 128, 256
TILES = D_MODEL // TC
LATER = 4
UP, DOWN = (3, 2, 1), (0, 1, 2)
T_X, T_D, T_W, T_G = 9, 10, 12, 30
NT_DIMS = (((1,), (1,)), ((), ()))
TN_DIMS = (((0,), (0,)), ((), ()))


def inside(r, n):
    return (r >= 0) & (r < n)


def scaled(a, unit):
    return pl.multiple_of(a * unit, unit)


def comm_kernel(od, od5, oc, oy, oyc, wo, foca, focb, foya, foyb, foza, fozb,
                dkv, dkv_c, n_hbm, wq, wca, wcb, wya, wk, wv, x_hbm, dout_hbm, gain_ref,
                out0, out1, gain_out, gk, gv, wyb, wza, wzb,
                pbuf, upb, dnb, zb, yb, cz, cy, fb, xo, do, stage, gacc,
                la, wof, wob, ra, p0, dqo, dqr, kva, kvs, kvr, lhs, wtf, wtq, wtk, rd, p1, dkvb, nt, gst,
                psem, up_r, dn_r, z_r, y_r, c_r,
                up_s, dn_s, zu_s, zd_s, za_s, y_s, c_s, o_sem, l_sem, e_s, e_r, w_sem, wo_sem, n_sem, g_sem):
    dp = lax.axis_index("dp")
    t = lax.axis_index("tp")
    z, y, c = t // 4, (t // 2) % 2, t % 2
    j = t % 4

    def dev(zz, yy, cc):
        return (dp, zz * 4 + yy * 2 + cc)

    above, below = dev(lax.rem(z + 1, 4), y, c), dev(lax.rem(z + 3, 4), y, c)

    def remote(src, dst, ss, rs, device):
        return pltpu.make_async_remote_copy(src_ref=src, dst_ref=dst, send_sem=ss, recv_sem=rs,
                                            device_id=device, device_id_type=MESH)

    def rowcol(r):
        kk = lax.rem(r, PER)
        first = r < PER
        row = jnp.where(first, lax.rem(kk, RCH), kk // HALVES)
        half = jnp.where(first, kk // RCH, lax.rem(kk, HALVES))
        return row, scaled(half, CC)

    def p_copy(p, r):
        rr, cc = rowcol(r)
        return pltpu.make_async_copy(p.at[:, rr, :, pl.ds(cc, CC)], pbuf.at[lax.rem(r, DP)], psem.at[lax.rem(r, DP)])

    def p_start(r):
        @pl.when(r < PER)
        def _():
            p_copy(p0, r).start()

        @pl.when((r >= PER) & (r < R))
        def _():
            p_copy(p1, r).start()

    def line_copy(buf, src, r, o, i, ss, rs, device):
        s = lax.rem(r, DR)
        return remote(pbuf.at[lax.rem(r, DP), o] if src is None else src.at[s, o], buf.at[s, o], ss.at[o, lax.rem(i, DS)], rs.at[o, s], device)

    def up_copy(r, o, i, src=upb):
        return line_copy(upb, src, r, o, i, up_s, up_r, above)

    def dn_copy(r, o, i, src=dnb):
        return line_copy(dnb, src, r, o, i, dn_s, dn_r, below)

    def cut(ref, small):
        return ref.at[:, pl.ds(0, GC)] if small else ref

    def along_z(r, q, i, small, sem, device):
        v = cut(zb.at[lax.rem(r, D), q], small)
        return remote(v, v, sem.at[lax.rem(i, DS)], z_r.at[q, lax.rem(r, D)], device)

    def y_copy(r, q, i, small, late):
        s = lax.rem(r, D)
        return remote(cut(zb.at[s, q], small), cut(yb.at[s, q], small), y_s.at[late, q, lax.rem(i, DS)], y_r.at[q, s], dev(z, 1 - y, c))

    def c_copy(k, r, i, small, late):
        s = lax.rem(r, D)
        src, dst = ((zb, cz), (yb, cy))[k]
        src, dst = src.at[s], dst.at[s]
        if small:
            src, dst = src.at[:, :, pl.ds(0, GC)], dst.at[:, :, pl.ds(0, GC)]
        return remote(src, dst, c_s.at[late, k, lax.rem(i, DS)], c_r.at[k, s], dev(z, y, 1 - c))

    def sized(i, delay, quick, f):
        @pl.when(inside(i - delay, L))
        def _():
            f(i - delay, False, 0)

        for small in (False, True):
            @pl.when(i - quick == L + small)
            def _():
                f(i - quick, small, 1)

    bufs = (zb, yb, cz, cy)

    def src_j(k):
        yy = y if k in (0, 2) else 1 - y
        cc = c if k in (0, 1) else 1 - c
        return yy * 2 + cc

    def o_copy(out, r, b, k):
        rr, cc = rowcol(r)
        return pltpu.make_async_copy(stage.at[b, k], out.at[src_j(k), :, rr, :, pl.ds(cc, CC)], o_sem.at[b, k])

    def when_line(i, hop, order, mine, make, f):
        r = i - hop
        for o in order:
            @pl.when(inside(r, R) & mine(o))
            def _():
                @pl.when(hop == 0)
                def _():
                    f(make(r, o, i, None))

                @pl.when(hop > 0)
                def _():
                    f(make(r, o, i))

    def when_sums(i, f):
        when_line(i, z, UP, lambda o: z < o, up_copy, f)
        when_line(i, 3 - z, DOWN, lambda o: z > o, dn_copy, f)

    def gathered_at(q):
        h = jnp.abs(z - q)
        return OWN + h, OWN + jnp.minimum(h, 1)

    def when_ag(i, q, f):
        def sends(r, small, late):
            if late:
                @pl.when(z == q)
                def _():
                    for d in UP:
                        f(along_z(r, q, i, small, za_s.at[d - 1], dev(lax.rem(z + d, 4), y, c)))
            else:
                @pl.when((z >= q) & (z < 3))
                def _():
                    f(along_z(r, q, i, small, zu_s.at[q], above))

                @pl.when((z <= q) & (z > 0))
                def _():
                    f(along_z(r, q, i, small, zd_s.at[q], below))

            f(y_copy(r, q, i, small, late))

        sized(i, *gathered_at(q), sends)

    def when_c(i, f):
        for k, at in enumerate((CSEND, YSEND)):
            sized(i, at, at - QUICK, lambda r, small, late: f(c_copy(k, r, i, small, late)))

    def head_at(p):
        return pl.ds(scaled(dp ^ p, HD), HD)

    def rows_of(jj):
        return pl.ds(scaled(jj, ROWS), ROWS)

    def wo_loads(n):
        b = lax.rem(n, 2)
        cols = pl.ds(scaled(n, TC), TC)
        cps = [(src.at[:, cols], wof.at[b, k]) for k, src in enumerate((foca, focb, foya, foyb, foza, fozb))] + [(wo.at[:, cols], wob.at[b])]
        return [pltpu.make_async_copy(a, v, wo_sem.at[b, k]) for k, (a, v) in enumerate(cps)]

    def first_tile(n):
        b = lax.rem(n, 2)
        for cp in wo_loads(n):
            cp.wait()
        for p in TWO:
            ra[p * HD:(p + 1) * HD, :] = wob[b, head_at(p), :]
        for k in SIX:
            ra[(2 + k) * HD:(3 + k) * HD, :] = wof[b, k].astype(BF16)
        tile = jnp.dot(la[...], ra[...], preferred_element_type=F32)
        p0[:, :, :, pl.ds(scaled(n, TC), TC)] = tile.reshape(4, RCH, CR, TC)

    def dq_send(d):
        return remote(od.at[pl.ds(2, 2), rows_of(j ^ d)], dqr.at[d - 1], e_s.at[d - 1], e_r.at[d - 1], (dp, t ^ d))

    exchange = [dq_send(1), dq_send(2), dq_send(3),
                remote(kvs.at[0], kvr, e_s.at[3], e_r.at[3], (dp, t ^ 2)),
                remote(wya, wyb, e_s.at[4], e_r.at[4], (1 - dp, t)),
                remote(wya, wza, e_s.at[5], e_r.at[5], (dp, t ^ 1))]
    last = remote(wyb, wzb, e_s.at[6], e_r.at[6], (dp, t ^ 1))
    own = pltpu.make_async_copy(od.at[pl.ds(2, 2), rows_of(j)], dqo, l_sem.at[2])

    def kv_loads(m):
        rows = rows_of(j ^ 2 ^ m)
        return [pltpu.make_async_copy(src.at[rows], kva.at[k], l_sem.at[3 + k]) for k, src in enumerate((dkv, dkv_c))]

    def kv_sum(m, out):
        for cp in kv_loads(m):
            cp.wait()
        total = kva[0] + kva[1]
        dkvb[rows_of(j ^ 2 ^ m), :] = total.astype(BF16)
        if out < 2:
            kvs[out] = total

    kv_own = t // 2

    def tile_loads(n):
        b = lax.rem(n, 2)
        r = pl.ds(scaled(n, TC), TC)
        cps = [(src.at[r], wtf.at[b, k]) for k, src in enumerate((wca, wcb, wya, wyb, wza, wzb))] + [(wq.at[r], wtq.at[b])]
        cps += [(src.at[r, pl.ds(scaled(h, HD), HD)], wtk.at[b, k])
                for k, (src, h) in enumerate(((wk, kv_own), (wv, kv_own), (wk, kv_own ^ 1), (wv, kv_own ^ 1)))]
        return [pltpu.make_async_copy(a, v, w_sem.at[b, k]) for k, (a, v) in enumerate(cps)]

    def second_tile(n):
        b = lax.rem(n, 2)
        for cp in tile_loads(n):
            cp.wait()
        for p in TWO:
            rd[:, p * HD:(p + 1) * HD] = wtq[b, :, head_at(p)]
        for k in SIX:
            rd[:, (2 + k) * HD:(3 + k) * HD] = wtf[b, k].astype(BF16)
        for k in FOUR:
            rd[:, (8 + k) * HD:(9 + k) * HD] = wtk[b, k]
        tile = lax.dot_general(lhs[...], rd[...], NT_DIMS, preferred_element_type=F32)
        p1[:, :, :, pl.ds(scaled(n, TC), TC)] = tile.reshape(4, RCH, CR, TC)

    def n_load(n):
        b = lax.rem(n, 2)
        return pltpu.make_async_copy(n_hbm.at[:, pl.ds(scaled(n, TC), TC)], nt.at[b], n_sem.at[b])

    def g_store(n):
        b = lax.rem(n, 2)
        r = pl.ds(scaled(n, TC), TC)
        return [pltpu.make_async_copy(gst.at[b, k], g.at[r], g_sem.at[b, k]) for k, g in enumerate((gk, gv))]

    def grad_tile(n):
        b = lax.rem(n, 2)
        n_load(n).wait()
        tile = lax.dot_general(nt[b], dkvb[...], TN_DIMS, preferred_element_type=F32)
        for k in TWO:
            gst[b, k] = tile[:, k * HD:(k + 1) * HD]
        for cp in g_store(n):
            cp.start()

    base = (j * 4 + z) * RCH
    owned = [pltpu.make_async_copy(x_hbm.at[pl.ds(base, RCH)], xo, l_sem.at[0]),
             pltpu.make_async_copy(dout_hbm.at[pl.ds(base, RCH)], do, l_sem.at[1])]

    def products(i):
        blocks = (0, 2, 1, 3)
        for at in FOUR:
            @pl.when(i == at + 1)
            def _():
                kv_sum(blocks[at], at)
                for m in blocks[at + 1:at + 2]:
                    for cp in kv_loads(m):
                        cp.start()

        @pl.when(i == 2)
        def _():
            exchange[3].start()
            for cp in owned:
                cp.wait()

        n = i + TILES // 2 - LATER

        @pl.when((i >= LATER) & (n + 1 < TILES))
        def _():
            for cp in wo_loads(n + 1):
                cp.start()

        @pl.when((i >= LATER) & (n < TILES))
        def _():
            first_tile(n)

        @pl.when(i == T_X)
        def _():
            exchange[4].wait()
            last.start()

        @pl.when(i == T_D)
        def _():
            for cp in [own] + exchange[:4] + exchange[5:]:
                cp.wait()
            for p in TWO:
                lhs[:, p * HD:(p + 1) * HD] = dqo[p].astype(BF16)
                for k in range(3):
                    lhs[:, (2 * k + 2 + p) * HD:(2 * k + 3 + p) * HD] = dqr[k, p].astype(BF16)
            lhs[:, 8 * HD:10 * HD] = kvs[1].astype(BF16)
            lhs[:, 10 * HD:] = kvr[...].astype(BF16)

        @pl.when(i == T_W)
        def _():
            last.wait()

        @pl.when(inside(i - T_W, TILES))
        def _():
            for cp in tile_loads(i - T_W):
                cp.start()

        @pl.when(inside(i - T_W - 1, TILES))
        def _():
            second_tile(i - T_W - 1)

        @pl.when(inside(i - T_G, TILES))
        def _():
            n_load(i - T_G).start()

        @pl.when(inside(i - T_G - 3, TILES))
        def _():
            for cp in g_store(i - T_G - 3):
                cp.wait()

        @pl.when(inside(i - T_G - 1, TILES))
        def _():
            grad_tile(i - T_G - 1)

    for cp in exchange[:3] + exchange[4:] + [own] + kv_loads(0):
        cp.start()
    loads = [pltpu.make_async_copy(src.at[p], p0.at[:, :, :, pl.ds((2 * k + p) * HD, HD)], l_sem.at[5 + 2 * k + p])
              for k, src in enumerate((od5.at[:, pl.ds(j * 4, 4)], oc, oy, oyc)) for p in TWO]
    for cp in loads + wo_loads(0) + owned:
        cp.start()
    gacc[...] = jnp.zeros_like(gacc)
    for cp in loads:
        cp.wait()
    for k in FOUR:
        for p in TWO:
            at = slice((2 * k + p) * HD, (2 * k + p + 1) * HD)
            la[:, at] = p0[:, :, :, at].reshape(ROWS, HD).astype(BF16)

    def first_half(n, _):
        for cp in wo_loads(n + 1):
            cp.start()
        first_tile(n)
        return 0

    lax.fori_loop(0, TILES // 2, first_half, 0)
    p_start(0)
    p_start(1)

    def body(i, _):
        products(i)

        ip = i - LAG

        @pl.when(ip >= 0)
        def _():
            when_sums(ip, lambda cp: cp.wait_send())
            for q in FOUR:
                when_ag(ip, q, lambda cp: cp.wait_send())
            when_c(ip, lambda cp: cp.wait_send())

        p_start(i + 2)

        @pl.when(i < R)
        def _():
            p_copy(p0, i).wait()

        def take(r, hop, order, make, buf, past):
            @pl.when(inside(r, R) & (hop > 0))
            def _():
                for o in order:
                    @pl.when(past(o))
                    def _():
                        make(r, o, i).wait_recv()
                        buf[lax.rem(r, DR), o] += pbuf[lax.rem(r, DP), o]

        take(i - z, z, UP, up_copy, upb, lambda o: z < o)
        take(i - 3 + z, 3 - z, DOWN, dn_copy, dnb, lambda o: z > o)

        rf = i - 3
        fs = lax.rem(rf, 2)

        @pl.when(inside(rf, R))
        def _():
            fb[fs] = pbuf[lax.rem(rf, DP), z]

            @pl.when(z > 0)
            def _():
                up_copy(rf, z, i).wait_recv()
                fb[fs] += upb[lax.rem(rf, DR), z]

            @pl.when(z < 3)
            def _():
                dn_copy(rf, z, i).wait_recv()
                fb[fs] += dnb[lax.rem(rf, DR), z]

            rr, cc = rowcol(rf)

            @pl.when(rf < PER)
            def _():
                zb[lax.rem(rf, D), z] = (xo[rr, :, pl.ds(cc, CC)].astype(F32) + fb[fs]).astype(BF16).astype(F32)

            @pl.when((rf >= PER) & (fs == 1))
            def _():
                xr = xo[rr].astype(F32)
                inv = lax.rsqrt(jnp.mean(xr * xr, axis=-1, keepdims=True) + NORM_EPS)
                u = xr * inv
                dn = jnp.concatenate([fb[0], fb[1]], axis=1)
                gg = dn * gain_ref[...]
                m = jnp.mean(gg * u, axis=-1, keepdims=True)
                dx = (do[rr].astype(F32) + inv * (gg - u * m)).astype(BF16).astype(F32)
                gacc[...] += dn * u
                zb[lax.rem(rf - 1, D), z] = dx[:, :CC]
                zb[lax.rem(rf, D), z] = dx[:, CC:]

        @pl.when(rf == R)
        def _():
            total = jnp.sum(gacc[...], axis=0, keepdims=True)
            zb[R % D, z, :, :GC] = jnp.concatenate([total[:, a * GC:(a + 1) * GC] for a in range(CR)], axis=0)

        when_sums(i, lambda cp: cp.start())

        for q in FOUR:
            @pl.when(z != q)
            def _():
                sized(i, *gathered_at(q), lambda r, small, late: along_z(r, q, i, small, zu_s.at[q], above).wait_recv())

            when_ag(i, q, lambda cp: cp.start())

        for q in FOUR:
            sized(i, YSEND, YSEND - QUICK, lambda r, small, late: y_copy(r, q, i, small, late).wait_recv())

        when_c(i, lambda cp: cp.start())

        def stored(i, f):
            r = i - CONV

            @pl.when(inside(r, PER))
            def _():
                f(out0, r, lax.rem(i, 2))

            @pl.when((r >= PER) & (r < L))
            def _():
                f(out1, r, lax.rem(i, 2))

            @pl.when(r + QUICK == L)
            def _():
                f(out1, L, 2)

        def wait_stored(out, r, b):
            for k in FOUR:
                o_copy(out, r, b, k).wait()

        def store(out, r, b):
            for k in FOUR:
                for q in FOUR:
                    stage[b, k, q] = bufs[k][lax.rem(r, D), q].astype(BF16)
                o_copy(out, r, b, k).start()

        stored(i - 2, wait_stored)
        for k in TWO:
            sized(i, CONV, CONV - QUICK, lambda r, small, late: c_copy(k, r, i, small, late).wait_recv())
        stored(i, store)

        @pl.when(i == R + CONV - QUICK)
        def _():
            acc = jnp.zeros((CR, GC), F32)
            for k in FOUR:
                for q in FOUR:
                    acc = acc + bufs[k][R % D, q, :, :GC]
            for h in range(CR):
                for a in range(GC // HD):
                    gain_out[h * (GC // HD) + a] = acc[h, a * HD:(a + 1) * HD]

        return 0

    lax.fori_loop(0, NI, body, 0)


def comm(od, os, wo, fos, dkv, dkv_c, n, wq, wqs, wk, wv, x, dout, gain):
    anyspec = pl.BlockSpec(memory_space=pl.ANY)
    hbm = pl.BlockSpec(memory_space=pltpu.HBM)
    vm = pl.BlockSpec(memory_space=pltpu.VMEM)
    dma, vmem, sds = pltpu.SemaphoreType.DMA, pltpu.VMEM, jax.ShapeDtypeStruct
    ch = (CR, CC)
    full = sds((4, 4, RCH, CR, D_MODEL), BF16)
    land = sds((D_MODEL, HD), F32)
    part = vmem((4, RCH, CR, D_MODEL), F32)
    owned = vmem((RCH, CR, D_MODEL), BF16)
    gathered = vmem((D, 4) + ch, F32)
    line = vmem((DR, 4) + ch, F32)
    pair = vmem((2, ROWS, 2 * HD), F32)
    return pl.pallas_call(
        comm_kernel,
        out_shape=(full, full, sds((D_MODEL // HD, HD), F32)) + (land,) * 5,
        in_specs=[hbm] * 23 + [vm],
        out_specs=(anyspec, anyspec, vm) + (hbm,) * 5,
        scratch_shapes=[
            vmem((DP, 4) + ch, F32), line, line, gathered, gathered, gathered, gathered, vmem((2,) + ch, F32),
            owned, owned, vmem((3, 4, 4) + ch, BF16), vmem((CR, D_MODEL), F32),
            vmem((ROWS, 8 * HD), BF16), vmem((2, 6, HD, TC), F32), vmem((2, 2 * HD, TC), BF16),
            vmem((8 * HD, TC), BF16), part,
            vmem((2, ROWS, HD), F32), vmem((3, 2, ROWS, HD), F32), pair, pair, vmem((ROWS, 2 * HD), F32),
            vmem((ROWS, 12 * HD), BF16), vmem((2, 6, TC, HD), F32), vmem((2, TC, 2 * HD), BF16), vmem((2, 4, TC, HD), BF16),
            vmem((TC, 12 * HD), BF16), part,
            vmem((4 * ROWS, 2 * HD), BF16), vmem((2, 4 * ROWS, TC), BF16), vmem((2, 2, TC, HD), F32),
            dma((DP,)), dma((4, DR)), dma((4, DR)), dma((4, D)), dma((4, D)), dma((2, D)),
            *[dma((4, DS))] * 5, dma((2, 4, DS)), dma((2, 2, DS)), dma((3, 4)), dma((13,)),
            dma((7,)), dma((7,)), dma((2, 11)), dma((2, 7)), dma((2,)), dma((2, 2)),
        ],
        compiler_params=pltpu.CompilerParams(has_side_effects=True, vmem_limit_bytes=62 * MIB),
        cost_estimate=pl.CostEstimate(flops=13 * 10**9, bytes_accessed=10**8, transcendentals=0),
        name="comm",
    )(od, od.reshape(4, 16, RCH, CR, HD), *[o.reshape(2, 4, RCH, CR, HD) for o in os], wo, *fos, dkv, dkv_c, n, wq, *wqs, wk, wv, x, dout, gain)[:5]


HEAD_DIM = 128
ROPE_BASE = 10000.0
SCORE_SCALE = 1.0 / math.sqrt(HEAD_DIM)
SEQ = 2048
NEG = -1.0e30 / SCORE_SCALE
TILE = 256


def mm(a, b):
    return jnp.dot(a, b, preferred_element_type=F32)


def mm_nt(a, b):
    return lax.dot_general(a, b, NT_DIMS, preferred_element_type=F32)


def widen_kernel(axis, dp_ref, w_ref, *outs):
    for p, out in enumerate(outs):
        at = pl.ds(scaled(dp_ref[0] ^ p, HEAD_DIM), HEAD_DIM)
        out[...] = (w_ref[:, at] if axis else w_ref[at, :]).astype(F32)


def widen(dp, w, axis):
    tile = 2048
    shape = lambda width: (tile, width) if axis else (width, tile)
    index = (lambda i, s: (i, 0)) if axis else (lambda i, s: (0, i))
    half = jax.ShapeDtypeStruct((D_MODEL, HEAD_DIM) if axis else (HEAD_DIM, D_MODEL), F32)
    return pl.pallas_call(
        functools.partial(widen_kernel, axis),
        grid_spec=pltpu.PrefetchScalarGridSpec(
            num_scalar_prefetch=1, grid=(D_MODEL // tile,),
            in_specs=[pl.BlockSpec(shape(2 * HEAD_DIM), index)],
            out_specs=(pl.BlockSpec(shape(HEAD_DIM), index),) * len(TWO)),
        out_shape=(half,) * len(TWO),
        cost_estimate=pl.CostEstimate(flops=10**9, bytes_accessed=6 * MIB, transcendentals=0),
        name="widen")(dp, w)


def swap_pairs(v):
    lane = lax.broadcasted_iota(jnp.int32, v.shape, 1)
    return jnp.where(lane % 2 == 0, pltpu.roll(v, HEAD_DIM - 1, 1), pltpu.roll(v, 1, 1))


def rotate(v, cos_v, sin_v):
    return v * cos_v + swap_pairs(v) * sin_v


def tile_angles(cos_ref, sin_ref, i):
    at = pl.ds(TILE + i, 1)
    ca, sa = cos_ref[at, :], sin_ref[at, :]
    cb, sb = cos_ref[:TILE, :], sin_ref[:TILE, :]
    even = lax.broadcasted_iota(jnp.int32, (TILE, HEAD_DIM), 1) % 2 == 0
    s = sa * cb + ca * sb
    return ca * cb - sa * sb, jnp.where(even, -s, s)


def proj_kernel(kv_ref, x_ref, dout_ref, gain_ref, wq_ref, wk_ref, wv_ref, wo_ref, cos_ref, sin_ref,
                n_ref, q_ref, k_ref, v_ref, do_ref, wkv):
    @pl.when(pl.program_id(0) == 0)
    def _():
        wkv[:, :HEAD_DIM] = wk_ref[...]
        wkv[:, HEAD_DIM:] = wv_ref[...]

    xf = x_ref[...].astype(F32)
    inv = lax.rsqrt(jnp.mean(xf * xf, axis=-1, keepdims=True) + NORM_EPS)
    n_ref[...] = (xf * inv * gain_ref[...]).astype(BF16)
    n = n_ref[...]
    q = mm(n, wq_ref[...])
    kv = mm(n, wkv[...])
    d = mm_nt(dout_ref[...], wo_ref[...])
    cos_v, sin_v = tile_angles(cos_ref, sin_ref, pl.program_id(0))
    for h in TWO:
        cols = slice(h * HEAD_DIM, (h + 1) * HEAD_DIM)
        q_ref[h] = rotate(q[:, cols], cos_v, sin_v).astype(BF16)
        do_ref[h] = d[:, cols].astype(BF16)
    k_ref[...] = rotate(kv[:, :HEAD_DIM], cos_v, sin_v).astype(BF16)
    v_ref[...] = kv[:, HEAD_DIM:].astype(BF16)


def proj(kv, x, dout, gain, w_query, w_key, w_value, w_out, cos_t, sin_t):
    row = lambda w: pl.BlockSpec((TILE, w), lambda i, s: (i, 0))
    whole = lambda a, b: pl.BlockSpec((a, b), lambda i, s: (0, 0))
    head2 = pl.BlockSpec((2, TILE, HEAD_DIM), lambda i, s: (0, i, 0))
    wspec = pl.BlockSpec((D_MODEL, HEAD_DIM), lambda i, s: (0, s[0]))
    sds = jax.ShapeDtypeStruct
    return pl.pallas_call(
        proj_kernel,
        grid_spec=pltpu.PrefetchScalarGridSpec(
            num_scalar_prefetch=1, grid=(SEQ // TILE,),
            in_specs=[row(D_MODEL), row(D_MODEL), whole(1, D_MODEL), whole(D_MODEL, 2 * HEAD_DIM), wspec, wspec,
                      whole(2 * HEAD_DIM, D_MODEL)] + [whole(TILE + SEQ // TILE, HEAD_DIM)] * 2,
            out_specs=(row(D_MODEL), head2, row(HEAD_DIM), row(HEAD_DIM), head2),
            scratch_shapes=[pltpu.VMEM((D_MODEL, 2 * HEAD_DIM), BF16)]),
        out_shape=(sds((SEQ, D_MODEL), BF16), sds((2, SEQ, HEAD_DIM), BF16), sds((SEQ, HEAD_DIM), BF16),
                   sds((SEQ, HEAD_DIM), BF16), sds((2, SEQ, HEAD_DIM), BF16)),
        compiler_params=pltpu.CompilerParams(vmem_limit_bytes=56 * MIB),
        cost_estimate=pl.CostEstimate(flops=2 * SEQ * D_MODEL * 768, bytes_accessed=58 * MIB, transcendentals=0),
        name="proj")(kv, x, dout, gain, w_query, w_key, w_value, w_out, cos_t, sin_t)


def attn_kernel(first, nt, dp_ref, q_ref, do_ref, k_ref, v_ref, cos_ref, sin_ref, *refs):
    prev, (o_ref, dq_ref, od_ref, dkv_ref, kt, vt, qt, dot_, qc, dc, s) = refs[:-11], refs[-11:]
    i = pl.program_id(0) + first
    wide = 2 * TILE
    c2 = SCORE_SCALE * math.log2(math.e)

    @pl.when(i == first)
    def _():
        def turn(b, _):
            r = pl.ds(pl.multiple_of(b * TILE, TILE), TILE)
            kt[b] = k_ref[r, :].T
            vt[b] = v_ref[r, :].T
            dkv_ref[r, :] = prev[-1][r, :] if prev else jnp.zeros((TILE, 2 * HEAD_DIM), F32)
            return 0

        lax.fori_loop(0, nt, turn, 0)

    for h in TWO:
        r = slice(h * TILE, (h + 1) * TILE)
        qc[r, :] = q_ref[h]
        dc[r, :] = do_ref[h]
        qt[:, r] = q_ref[h].T
        dot_[:, r] = do_ref[h].T

    def keys(b):
        return pl.ds(pl.multiple_of(b * TILE, TILE), TILE)

    def fold(f, v):
        a = v[:8]
        for g in range(1, TILE // 8):
            a = f(a, v[g * 8:(g + 1) * 8])
        return a

    def score(b, m):
        sb = mm(k_ref[keys(b), :], qt[...])
        s[b] = sb
        return jnp.maximum(m, fold(jnp.maximum, sb))

    m8 = lax.fori_loop(0, i, score, jnp.full((8, wide), NEG, F32))
    sb = mm(k_ref[keys(i), :], qt[...])
    key = lax.broadcasted_iota(jnp.int32, (TILE, wide), 0)
    query = lax.broadcasted_iota(jnp.int32, (TILE, wide), 1) % TILE
    sb = jnp.where(key <= query, sb, NEG)
    s[i] = sb
    m8 = jnp.maximum(m8, fold(jnp.maximum, sb))
    m = jnp.max(m8, axis=0, keepdims=True) * c2

    def expo(b, l):
        p = jnp.exp2(s[b] * c2 - m)
        s[b] = p
        return l + fold(jnp.add, p)

    l8 = lax.fori_loop(0, i + 1, expo, jnp.zeros((8, wide), F32))
    inv_l = 1.0 / jnp.sum(l8, axis=0, keepdims=True)

    def value(b, acc):
        p = s[b] * inv_l
        s[b] = p
        return acc + mm(vt[b], p.astype(BF16))

    ot = lax.fori_loop(0, i + 1, value, jnp.zeros((HEAD_DIM, wide), F32))
    row_dot = jnp.sum(ot * dot_[...].astype(F32), axis=0, keepdims=True)

    def grads(b, acc):
        p = s[b]
        dp = mm(v_ref[keys(b), :], dot_[...])
        ds = (p * (dp - row_dot)).astype(BF16)
        dkv_ref[keys(b), :HEAD_DIM] += mm(ds, qc[...])
        dkv_ref[keys(b), HEAD_DIM:] += mm(p.astype(BF16), dc[...])
        return acc + mm(kt[b], ds)

    dqt = lax.fori_loop(0, i + 1, grads, jnp.zeros((HEAD_DIM, wide), F32))

    cos_v, sin_v = tile_angles(cos_ref, sin_ref, i)
    for h in TWO:
        cols = slice(h * HEAD_DIM, (h + 1) * HEAD_DIM)
        r = slice(h * TILE, (h + 1) * TILE)
        o = ot[:, r].T.astype(BF16)
        dq = rotate(dqt[:, r].T * SCORE_SCALE, cos_v, -sin_v).astype(BF16)
        o_ref[:, cols] = o
        dq_ref[:, cols] = dq
        place = dp_ref[0] ^ h
        od_ref[place] = o.astype(F32)
        od_ref[2 + place] = dq.astype(F32)

    if prev:
        @pl.when(i == nt - 1)
        def _():
            def finish(b, _):
                r = keys(b)
                cos_b, sin_b = tile_angles(cos_ref, sin_ref, b)
                dkv_ref[r, :HEAD_DIM] = rotate(dkv_ref[r, :HEAD_DIM] * SCORE_SCALE, cos_b, -sin_b)
                return 0

            lax.fori_loop(0, nt, finish, 0)


def attention(dp, q, do, k, v, cos_t, sin_t, first, count, prev):
    n = SEQ // TILE
    head2 = pl.BlockSpec((2, TILE, HEAD_DIM), lambda i, s: (0, i + first, 0))
    whole = pl.BlockSpec((SEQ, HEAD_DIM), lambda i, s: (0, 0))
    angle = pl.BlockSpec((TILE + n, HEAD_DIM), lambda i, s: (0, 0))
    both = pl.BlockSpec((TILE, 2 * HEAD_DIM), lambda i, s: (i + first, 0))
    sums = pl.BlockSpec((SEQ, 2 * HEAD_DIM), lambda i, s: (0, 0))
    sds, vmem = jax.ShapeDtypeStruct, pltpu.VMEM
    heads_t, turned, stacked = vmem((n, HEAD_DIM, TILE), BF16), vmem((HEAD_DIM, 2 * TILE), BF16), vmem((2 * TILE, HEAD_DIM), BF16)
    args = (dp, q, do, k, v, cos_t, sin_t)
    return pl.pallas_call(
        functools.partial(attn_kernel, first, n),
        grid_spec=pltpu.PrefetchScalarGridSpec(
            num_scalar_prefetch=1, grid=(count,),
            in_specs=[head2, head2, whole, whole, angle, angle] + ([pl.BlockSpec(memory_space=pl.ANY)] * 3 + [sums] if prev else []),
            out_specs=(both, both, pl.BlockSpec((4, TILE, HEAD_DIM), lambda i, s: (0, i + first, 0)), sums),
            scratch_shapes=[heads_t, heads_t, turned, turned, stacked, stacked, vmem((n, TILE, 2 * TILE), F32)]),
        out_shape=(sds((SEQ, 2 * HEAD_DIM), BF16), sds((SEQ, 2 * HEAD_DIM), BF16), sds((4, SEQ, HEAD_DIM), F32), sds((SEQ, 2 * HEAD_DIM), F32)),
        input_output_aliases={len(args) + a: a for a in range(len(prev))},
        compiler_params=pltpu.CompilerParams(vmem_limit_bytes=56 * MIB),
        cost_estimate=pl.CostEstimate(flops=6 * 10**9, bytes_accessed=14 * MIB, transcendentals=10**6),
        name="attention")(*args, *prev)


def rope_tables():
    lane = jnp.arange(HEAD_DIM)
    inv_freq = ROPE_BASE ** (-(lane - lane % 2).astype(F32) / HEAD_DIM)
    rows = jnp.concatenate([jnp.arange(TILE), jnp.arange(SEQ // TILE) * TILE]).astype(F32)
    angles = rows[:, None] * inv_freq[None, :]
    return jnp.cos(angles), jnp.sin(angles)


def block_fn(hidden, grad_out, norm_gain, w_query, w_key, w_value, w_out):
    seq_len, d_model = hidden.shape[1:]
    x, dout = hidden[0], grad_out[0]
    t = lax.axis_index('tp')
    dp = lax.axis_index('dp')
    j = t % 4
    rows = seq_len // 4
    pre = jnp.stack([dp, j, t // 2]).astype(jnp.int32)
    dpa, kva = pre[0:1], pre[2:3]

    def flip(v, d):
        return lax.ppermute(v, 'tp', [(s, s ^ d) for s in range(16)])

    def over_x(v):
        return lax.ppermute(v, 'dp', [(0, 1), (1, 0)])

    woa, wob = widen(dpa, w_out, 0)
    wo_ya = flip(woa, 2)
    wo_yb = over_x(wo_ya)
    fos = [flip(woa, 1), flip(wob, 1), wo_ya, wo_yb, flip(wo_ya, 1), flip(wo_yb, 1)]
    kva, w_query_, _ = lax.optimization_barrier((kva, w_query, woa))
    cos_t, sin_t = rope_tables()
    gain = norm_gain.astype(F32).reshape(1, d_model)
    n, q, k, v, do = proj(kva, x, dout, gain, w_query_, w_key, w_value, w_out, cos_t, sin_t)
    dpb, _ = lax.optimization_barrier((dpa, k))
    wqa, wqb = widen(dpb, w_query, 1)
    wqs = [flip(wqa, 1), flip(wqb, 1), flip(wqa, 2)]
    dpc, _ = lax.optimization_barrier((dpa, wqa))
    part = attention(dpc, q, do, k, v, cos_t, sin_t, 0, SEQ // TILE // 2, ())
    o, dq, od, dkv_part = attention(dpc, q, do, k, v, cos_t, sin_t, SEQ // TILE // 2, SEQ // TILE // 2, part)

    def rows_of(jj):
        return lax.dynamic_slice(od, (0, jj * rows, 0), (2, rows, HEAD_DIM))

    os = [flip(rows_of(j ^ d), d) for d in (1, 2, 3)]
    dkv_c = flip(dkv_part, 1)
    grad_w_query = jnp.einsum('sd,se->de', n, dq, preferred_element_type=F32)
    grad_w_out = jnp.einsum('se,sd->ed', o, dout, preferred_element_type=F32)

    tiles = (seq_len // CR, CR, d_model)
    out, dx, gg, gk, gv = comm(od, os, w_out, fos, dkv_part, dkv_c, n, w_query, wqs, w_key, w_value,
                               x.reshape(tiles), dout.reshape(tiles), gain)
    return (out.reshape(1, seq_len, d_model), dx.reshape(1, seq_len, d_model), gg.reshape(d_model), grad_w_query, gk, gv, grad_w_out)


def solution(mesh):
    act_spec = P('dp', None, None)

    return jax.shard_map(
        block_fn, mesh=mesh,
        in_specs=(act_spec, act_spec, P(None), P(None, 'tp'), P(None, None), P(None, None), P('tp', None)),
        out_specs=(act_spec, act_spec, P('dp'), P('dp', 'tp'), P('dp', 'tp'), P('dp', 'tp'), P(('dp', 'tp'), None)),
        check_vma=False)
```

```python
import functools
import math
import jax
import jax.numpy as jnp
from jax import lax
from jax.experimental import pallas as pl
from jax.experimental.pallas import tpu as pltpu
from jax.sharding import PartitionSpec as P

F32, BF16 = jnp.float32, jnp.bfloat16
MESH = pl.DeviceIdType.MESH
NORM_EPS = 1.0e-5
MIB = 2 ** 20
TWO, FOUR, SIX = range(2), range(4), range(6)
CR, CC = 8, 2048
GC = 512
D_MODEL = 4096
SHARD = 128
RCH = SHARD // CR
HALVES = D_MODEL // CC
PER = RCH * HALVES
R = 2 * PER
OWN, CSEND, YSEND, CONV = 4, 7, 8, 9
LAG = 3
L, QUICK = R - 1, 2
NI = R + CONV + 1
DP, DR, D, DS = 8, 8, 16, 4
ROWS, HD, TC = 512, 128, 256
TILES = D_MODEL // TC
LATER = 4
UP, DOWN = (3, 2, 1), (0, 1, 2)
T_X, T_D, T_W = 9, 10, 12
NT_DIMS = (((1,), (1,)), ((), ()))
TN_DIMS = (((0,), (0,)), ((), ()))


def inside(r, n):
    return (r >= 0) & (r < n)


def scaled(a, unit):
    return pl.multiple_of(a * unit, unit)


def comm_kernel(od, od5, oc, oy, oyc, wo, foca, focb, foya, foyb, foza, fozb,
                dkv, dkv_c, wq, wca, wcb, wya, wk, wv, x_hbm, dout_hbm, gain_ref,
                out0, out1, gain_out, wyb, wza, wzb,
                pbuf, upb, dnb, zb, yb, cz, cy, fb, xo, do, stage, gacc,
                la, wof, wob, ra, p0, dqo, dqr, kva, kvs, kvr, lhs, wtf, wtq, wtk, rd, p1,
                psem, up_r, dn_r, z_r, y_r, c_r,
                up_s, dn_s, zu_s, zd_s, za_s, y_s, c_s, o_sem, l_sem, e_s, e_r, w_sem, wo_sem):
    dp = lax.axis_index("dp")
    t = lax.axis_index("tp")
    z, y, c = t // 4, (t // 2) % 2, t % 2
    j = t % 4

    def dev(zz, yy, cc):
        return (dp, zz * 4 + yy * 2 + cc)

    above, below = dev(lax.rem(z + 1, 4), y, c), dev(lax.rem(z + 3, 4), y, c)

    def remote(src, dst, ss, rs, device):
        return pltpu.make_async_remote_copy(src_ref=src, dst_ref=dst, send_sem=ss, recv_sem=rs,
                                            device_id=device, device_id_type=MESH)

    def rowcol(r):
        kk = lax.rem(r, PER)
        first = r < PER
        row = jnp.where(first, lax.rem(kk, RCH), kk // HALVES)
        half = jnp.where(first, kk // RCH, lax.rem(kk, HALVES))
        return row, scaled(half, CC)

    def p_copy(p, r):
        rr, cc = rowcol(r)
        return pltpu.make_async_copy(p.at[:, rr, :, pl.ds(cc, CC)], pbuf.at[lax.rem(r, DP)], psem.at[lax.rem(r, DP)])

    def p_start(r):
        @pl.when(r < PER)
        def _():
            p_copy(p0, r).start()

        @pl.when((r >= PER) & (r < R))
        def _():
            p_copy(p1, r).start()

    def line_copy(buf, src, r, o, i, ss, rs, device):
        s = lax.rem(r, DR)
        return remote(pbuf.at[lax.rem(r, DP), o] if src is None else src.at[s, o], buf.at[s, o], ss.at[o, lax.rem(i, DS)], rs.at[o, s], device)

    def up_copy(r, o, i, src=upb):
        return line_copy(upb, src, r, o, i, up_s, up_r, above)

    def dn_copy(r, o, i, src=dnb):
        return line_copy(dnb, src, r, o, i, dn_s, dn_r, below)

    def cut(ref, small):
        return ref.at[:, pl.ds(0, GC)] if small else ref

    def along_z(r, q, i, small, sem, device):
        v = cut(zb.at[lax.rem(r, D), q], small)
        return remote(v, v, sem.at[lax.rem(i, DS)], z_r.at[q, lax.rem(r, D)], device)

    def y_copy(r, q, i, small, late):
        s = lax.rem(r, D)
        return remote(cut(zb.at[s, q], small), cut(yb.at[s, q], small), y_s.at[late, q, lax.rem(i, DS)], y_r.at[q, s], dev(z, 1 - y, c))

    def c_copy(k, r, i, small, late):
        s = lax.rem(r, D)
        src, dst = ((zb, cz), (yb, cy))[k]
        src, dst = src.at[s], dst.at[s]
        if small:
            src, dst = src.at[:, :, pl.ds(0, GC)], dst.at[:, :, pl.ds(0, GC)]
        return remote(src, dst, c_s.at[late, k, lax.rem(i, DS)], c_r.at[k, s], dev(z, y, 1 - c))

    def sized(i, delay, quick, f):
        @pl.when(inside(i - delay, L))
        def _():
            f(i - delay, False, 0)

        for small in (False, True):
            @pl.when(i - quick == L + small)
            def _():
                f(i - quick, small, 1)

    bufs = (zb, yb, cz, cy)

    def src_j(k):
        yy = y if k in (0, 2) else 1 - y
        cc = c if k in (0, 1) else 1 - c
        return yy * 2 + cc

    def o_copy(out, r, b, k):
        rr, cc = rowcol(r)
        return pltpu.make_async_copy(stage.at[b, k], out.at[src_j(k), :, rr, :, pl.ds(cc, CC)], o_sem.at[b, k])

    def when_line(i, hop, order, mine, make, f):
        r = i - hop
        for o in order:
            @pl.when(inside(r, R) & mine(o))
            def _():
                @pl.when(hop == 0)
                def _():
                    f(make(r, o, i, None))

                @pl.when(hop > 0)
                def _():
                    f(make(r, o, i))

    def when_sums(i, f):
        when_line(i, z, UP, lambda o: z < o, up_copy, f)
        when_line(i, 3 - z, DOWN, lambda o: z > o, dn_copy, f)

    def gathered_at(q):
        h = jnp.abs(z - q)
        return OWN + h, OWN + jnp.minimum(h, 1)

    def when_ag(i, q, f):
        def sends(r, small, late):
            if late:
                @pl.when(z == q)
                def _():
                    for d in UP:
                        f(along_z(r, q, i, small, za_s.at[d - 1], dev(lax.rem(z + d, 4), y, c)))
            else:
                @pl.when((z >= q) & (z < 3))
                def _():
                    f(along_z(r, q, i, small, zu_s.at[q], above))

                @pl.when((z <= q) & (z > 0))
                def _():
                    f(along_z(r, q, i, small, zd_s.at[q], below))

            f(y_copy(r, q, i, small, late))

        sized(i, *gathered_at(q), sends)

    def when_c(i, f):
        for k, at in enumerate((CSEND, YSEND)):
            sized(i, at, at - QUICK, lambda r, small, late: f(c_copy(k, r, i, small, late)))

    def head_at(p):
        return pl.ds(scaled(dp ^ p, HD), HD)

    def rows_of(jj):
        return pl.ds(scaled(jj, ROWS), ROWS)

    def wo_loads(n):
        b = lax.rem(n, 2)
        cols = pl.ds(scaled(n, TC), TC)
        cps = [(src.at[:, cols], wof.at[b, k]) for k, src in enumerate((foca, focb, foya, foyb, foza, fozb))] + [(wo.at[:, cols], wob.at[b])]
        return [pltpu.make_async_copy(a, v, wo_sem.at[b, k]) for k, (a, v) in enumerate(cps)]

    def first_tile(n):
        b = lax.rem(n, 2)
        for cp in wo_loads(n):
            cp.wait()
        for p in TWO:
            ra[p * HD:(p + 1) * HD, :] = wob[b, head_at(p), :]
        for k in SIX:
            ra[(2 + k) * HD:(3 + k) * HD, :] = wof[b, k].astype(BF16)
        tile = jnp.dot(la[...], ra[...], preferred_element_type=F32)
        p0[:, :, :, pl.ds(scaled(n, TC), TC)] = tile.reshape(4, RCH, CR, TC)

    def dq_send(d):
        return remote(od.at[pl.ds(2, 2), rows_of(j ^ d)], dqr.at[d - 1], e_s.at[d - 1], e_r.at[d - 1], (dp, t ^ d))

    exchange = [dq_send(1), dq_send(2), dq_send(3),
                remote(kvs.at[0], kvr, e_s.at[3], e_r.at[3], (dp, t ^ 2)),
                remote(wya, wyb, e_s.at[4], e_r.at[4], (1 - dp, t)),
                remote(wya, wza, e_s.at[5], e_r.at[5], (dp, t ^ 1))]
    last = remote(wyb, wzb, e_s.at[6], e_r.at[6], (dp, t ^ 1))
    own = pltpu.make_async_copy(od.at[pl.ds(2, 2), rows_of(j)], dqo, l_sem.at[2])

    def kv_loads(m):
        rows = rows_of(j ^ 2 ^ m)
        return [pltpu.make_async_copy(src.at[rows], kva.at[k], l_sem.at[3 + k]) for k, src in enumerate((dkv, dkv_c))]

    def kv_sum(m, out):
        for cp in kv_loads(m):
            cp.wait()
        kvs[out] = kva[0] + kva[1]

    kv_own = t // 2

    def tile_loads(n):
        b = lax.rem(n, 2)
        r = pl.ds(scaled(n, TC), TC)
        cps = [(src.at[r], wtf.at[b, k]) for k, src in enumerate((wca, wcb, wya, wyb, wza, wzb))] + [(wq.at[r], wtq.at[b])]
        cps += [(src.at[r, pl.ds(scaled(h, HD), HD)], wtk.at[b, k])
                for k, (src, h) in enumerate(((wk, kv_own), (wv, kv_own), (wk, kv_own ^ 1), (wv, kv_own ^ 1)))]
        return [pltpu.make_async_copy(a, v, w_sem.at[b, k]) for k, (a, v) in enumerate(cps)]

    def second_tile(n):
        b = lax.rem(n, 2)
        for cp in tile_loads(n):
            cp.wait()
        for p in TWO:
            rd[:, p * HD:(p + 1) * HD] = wtq[b, :, head_at(p)]
        for k in SIX:
            rd[:, (2 + k) * HD:(3 + k) * HD] = wtf[b, k].astype(BF16)
        for k in FOUR:
            rd[:, (8 + k) * HD:(9 + k) * HD] = wtk[b, k]
        tile = lax.dot_general(lhs[...], rd[...], NT_DIMS, preferred_element_type=F32)
        p1[:, :, :, pl.ds(scaled(n, TC), TC)] = tile.reshape(4, RCH, CR, TC)

    base = (j * 4 + z) * RCH
    owned = [pltpu.make_async_copy(x_hbm.at[pl.ds(base, RCH)], xo, l_sem.at[0]),
             pltpu.make_async_copy(dout_hbm.at[pl.ds(base, RCH)], do, l_sem.at[1])]

    def products(i):
        for at in TWO:
            @pl.when(i == at + 1)
            def _():
                kv_sum(2 * at, at)
                if at == 0:
                    for cp in kv_loads(2):
                        cp.start()

        @pl.when(i == 2)
        def _():
            exchange[3].start()
            for cp in owned:
                cp.wait()

        n = i + TILES // 2 - LATER

        @pl.when((i >= LATER) & (n + 1 < TILES))
        def _():
            for cp in wo_loads(n + 1):
                cp.start()

        @pl.when((i >= LATER) & (n < TILES))
        def _():
            first_tile(n)

        @pl.when(i == T_X)
        def _():
            exchange[4].wait()
            last.start()

        @pl.when(i == T_D)
        def _():
            for cp in [own] + exchange[:4] + exchange[5:]:
                cp.wait()
            for p in TWO:
                lhs[:, p * HD:(p + 1) * HD] = dqo[p].astype(BF16)
                for k in range(3):
                    lhs[:, (2 * k + 2 + p) * HD:(2 * k + 3 + p) * HD] = dqr[k, p].astype(BF16)
            lhs[:, 8 * HD:10 * HD] = kvs[1].astype(BF16)
            lhs[:, 10 * HD:] = kvr[...].astype(BF16)

        @pl.when(i == T_W)
        def _():
            last.wait()

        @pl.when(inside(i - T_W, TILES))
        def _():
            for cp in tile_loads(i - T_W):
                cp.start()

        @pl.when(inside(i - T_W - 1, TILES))
        def _():
            second_tile(i - T_W - 1)

    for cp in exchange[:3] + exchange[4:] + [own] + kv_loads(0):
        cp.start()
    loads = [pltpu.make_async_copy(src.at[p], p0.at[:, :, :, pl.ds((2 * k + p) * HD, HD)], l_sem.at[5 + 2 * k + p])
              for k, src in enumerate((od5.at[:, pl.ds(j * 4, 4)], oc, oy, oyc)) for p in TWO]
    for cp in loads + wo_loads(0) + owned:
        cp.start()
    gacc[...] = jnp.zeros_like(gacc)
    for cp in loads:
        cp.wait()
    for k in FOUR:
        for p in TWO:
            at = slice((2 * k + p) * HD, (2 * k + p + 1) * HD)
            la[:, at] = p0[:, :, :, at].reshape(ROWS, HD).astype(BF16)

    def first_half(n, _):
        for cp in wo_loads(n + 1):
            cp.start()
        first_tile(n)
        return 0

    lax.fori_loop(0, TILES // 2, first_half, 0)
    p_start(0)
    p_start(1)

    def body(i, _):
        products(i)

        ip = i - LAG

        @pl.when(ip >= 0)
        def _():
            when_sums(ip, lambda cp: cp.wait_send())
            for q in FOUR:
                when_ag(ip, q, lambda cp: cp.wait_send())
            when_c(ip, lambda cp: cp.wait_send())

        p_start(i + 2)

        @pl.when(i < R)
        def _():
            p_copy(p0, i).wait()

        def take(r, hop, order, make, buf, past):
            @pl.when(inside(r, R) & (hop > 0))
            def _():
                for o in order:
                    @pl.when(past(o))
                    def _():
                        make(r, o, i).wait_recv()
                        buf[lax.rem(r, DR), o] += pbuf[lax.rem(r, DP), o]

        take(i - z, z, UP, up_copy, upb, lambda o: z < o)
        take(i - 3 + z, 3 - z, DOWN, dn_copy, dnb, lambda o: z > o)

        rf = i - 3
        fs = lax.rem(rf, 2)

        @pl.when(inside(rf, R))
        def _():
            fb[fs] = pbuf[lax.rem(rf, DP), z]

            @pl.when(z > 0)
            def _():
                up_copy(rf, z, i).wait_recv()
                fb[fs] += upb[lax.rem(rf, DR), z]

            @pl.when(z < 3)
            def _():
                dn_copy(rf, z, i).wait_recv()
                fb[fs] += dnb[lax.rem(rf, DR), z]

            rr, cc = rowcol(rf)

            @pl.when(rf < PER)
            def _():
                zb[lax.rem(rf, D), z] = (xo[rr, :, pl.ds(cc, CC)].astype(F32) + fb[fs]).astype(BF16).astype(F32)

            @pl.when((rf >= PER) & (fs == 1))
            def _():
                xr = xo[rr].astype(F32)
                inv = lax.rsqrt(jnp.mean(xr * xr, axis=-1, keepdims=True) + NORM_EPS)
                u = xr * inv
                dn = jnp.concatenate([fb[0], fb[1]], axis=1)
                gg = dn * gain_ref[...]
                m = jnp.mean(gg * u, axis=-1, keepdims=True)
                dx = (do[rr].astype(F32) + inv * (gg - u * m)).astype(BF16).astype(F32)
                gacc[...] += dn * u
                zb[lax.rem(rf - 1, D), z] = dx[:, :CC]
                zb[lax.rem(rf, D), z] = dx[:, CC:]

        @pl.when(rf == R)
        def _():
            total = jnp.sum(gacc[...], axis=0, keepdims=True)
            zb[R % D, z, :, :GC] = jnp.concatenate([total[:, a * GC:(a + 1) * GC] for a in range(CR)], axis=0)

        when_sums(i, lambda cp: cp.start())

        for q in FOUR:
            @pl.when(z != q)
            def _():
                sized(i, *gathered_at(q), lambda r, small, late: along_z(r, q, i, small, zu_s.at[q], above).wait_recv())

            when_ag(i, q, lambda cp: cp.start())

        for q in FOUR:
            sized(i, YSEND, YSEND - QUICK, lambda r, small, late: y_copy(r, q, i, small, late).wait_recv())

        when_c(i, lambda cp: cp.start())

        def stored(i, f):
            r = i - CONV

            @pl.when(inside(r, PER))
            def _():
                f(out0, r, lax.rem(i, 2))

            @pl.when((r >= PER) & (r < L))
            def _():
                f(out1, r, lax.rem(i, 2))

            @pl.when(r + QUICK == L)
            def _():
                f(out1, L, 2)

        def wait_stored(out, r, b):
            for k in FOUR:
                o_copy(out, r, b, k).wait()

        def store(out, r, b):
            for k in FOUR:
                for q in FOUR:
                    stage[b, k, q] = bufs[k][lax.rem(r, D), q].astype(BF16)
                o_copy(out, r, b, k).start()

        stored(i - 2, wait_stored)
        for k in TWO:
            sized(i, CONV, CONV - QUICK, lambda r, small, late: c_copy(k, r, i, small, late).wait_recv())
        stored(i, store)

        @pl.when(i == R + CONV - QUICK)
        def _():
            acc = jnp.zeros((CR, GC), F32)
            for k in FOUR:
                for q in FOUR:
                    acc = acc + bufs[k][R % D, q, :, :GC]
            for h in range(CR):
                for a in range(GC // HD):
                    gain_out[h * (GC // HD) + a] = acc[h, a * HD:(a + 1) * HD]

        return 0

    lax.fori_loop(0, NI, body, 0)


def comm(od, os, wo, fos, dkv, dkv_c, wq, wqs, wk, wv, x, dout, gain):
    anyspec = pl.BlockSpec(memory_space=pl.ANY)
    hbm = pl.BlockSpec(memory_space=pltpu.HBM)
    vm = pl.BlockSpec(memory_space=pltpu.VMEM)
    dma, vmem, sds = pltpu.SemaphoreType.DMA, pltpu.VMEM, jax.ShapeDtypeStruct
    ch = (CR, CC)
    full = sds((4, 4, RCH, CR, D_MODEL), BF16)
    land = sds((D_MODEL, HD), F32)
    part = vmem((4, RCH, CR, D_MODEL), F32)
    owned = vmem((RCH, CR, D_MODEL), BF16)
    gathered = vmem((D, 4) + ch, F32)
    line = vmem((DR, 4) + ch, F32)
    pair = vmem((2, ROWS, 2 * HD), F32)
    return pl.pallas_call(
        comm_kernel,
        out_shape=(full, full, sds((D_MODEL // HD, HD), F32)) + (land,) * 3,
        in_specs=[hbm] * 22 + [vm],
        out_specs=(anyspec, anyspec, vm) + (hbm,) * 3,
        scratch_shapes=[
            vmem((DP, 4) + ch, F32), line, line, gathered, gathered, gathered, gathered, vmem((2,) + ch, F32),
            owned, owned, vmem((3, 4, 4) + ch, BF16), vmem((CR, D_MODEL), F32),
            vmem((ROWS, 8 * HD), BF16), vmem((2, 6, HD, TC), F32), vmem((2, 2 * HD, TC), BF16),
            vmem((8 * HD, TC), BF16), part,
            vmem((2, ROWS, HD), F32), vmem((3, 2, ROWS, HD), F32), pair, pair, vmem((ROWS, 2 * HD), F32),
            vmem((ROWS, 12 * HD), BF16), vmem((2, 6, TC, HD), F32), vmem((2, TC, 2 * HD), BF16), vmem((2, 4, TC, HD), BF16),
            vmem((TC, 12 * HD), BF16), part,
            dma((DP,)), dma((4, DR)), dma((4, DR)), dma((4, D)), dma((4, D)), dma((2, D)),
            *[dma((4, DS))] * 5, dma((2, 4, DS)), dma((2, 2, DS)), dma((3, 4)), dma((13,)),
            dma((7,)), dma((7,)), dma((2, 11)), dma((2, 7)),
        ],
        compiler_params=pltpu.CompilerParams(has_side_effects=True, vmem_limit_bytes=62 * MIB),
        cost_estimate=pl.CostEstimate(flops=13 * 10**9, bytes_accessed=10**8, transcendentals=0),
        name="comm",
    )(od, od.reshape(4, 16, RCH, CR, HD), *[o.reshape(2, 4, RCH, CR, HD) for o in os], wo, *fos, dkv, dkv_c, wq, *wqs, wk, wv, x, dout, gain)[:3]


HEAD_DIM = 128
ROPE_BASE = 10000.0
SCORE_SCALE = 1.0 / math.sqrt(HEAD_DIM)
SEQ = 2048
WT = 512
NEG = -1.0e30 / SCORE_SCALE
TILE, KEYS = 256, 512


def mm(a, b):
    return jnp.dot(a, b, preferred_element_type=F32)


def mm_nt(a, b):
    return lax.dot_general(a, b, NT_DIMS, preferred_element_type=F32)


def widen_kernel(axis, dp_ref, w_ref, *outs):
    for p, out in enumerate(outs):
        at = pl.ds(scaled(dp_ref[0] ^ p, HEAD_DIM), HEAD_DIM)
        out[...] = (w_ref[:, at] if axis else w_ref[at, :]).astype(F32)


def widen(dp, w, axis):
    tile = 2048
    shape = lambda width: (tile, width) if axis else (width, tile)
    index = (lambda i, s: (i, 0)) if axis else (lambda i, s: (0, i))
    half = jax.ShapeDtypeStruct((D_MODEL, HEAD_DIM) if axis else (HEAD_DIM, D_MODEL), F32)
    return pl.pallas_call(
        functools.partial(widen_kernel, axis),
        grid_spec=pltpu.PrefetchScalarGridSpec(
            num_scalar_prefetch=1, grid=(D_MODEL // tile,),
            in_specs=[pl.BlockSpec(shape(2 * HEAD_DIM), index)],
            out_specs=(pl.BlockSpec(shape(HEAD_DIM), index),) * len(TWO)),
        out_shape=(half,) * len(TWO),
        cost_estimate=pl.CostEstimate(flops=10**9, bytes_accessed=6 * MIB, transcendentals=0),
        name="widen")(dp, w)


def swap_pairs(v):
    lane = lax.broadcasted_iota(jnp.int32, v.shape, 1)
    return jnp.where(lane % 2 == 0, pltpu.roll(v, HEAD_DIM - 1, 1), pltpu.roll(v, 1, 1))


def rotate(v, cos_v, sin_v):
    return v * cos_v + swap_pairs(v) * sin_v


def tile_angles(cos_ref, sin_ref, i):
    at = pl.ds(TILE + i, 1)
    ca, sa = cos_ref[at, :], sin_ref[at, :]
    cb, sb = cos_ref[:TILE, :], sin_ref[:TILE, :]
    even = lax.broadcasted_iota(jnp.int32, (TILE, HEAD_DIM), 1) % 2 == 0
    s = sa * cb + ca * sb
    return ca * cb - sa * sb, jnp.where(even, -s, s)


def proj_kernel(kv_ref, x_ref, dout_ref, gain_ref, wq_ref, wk_ref, wv_ref, wo_ref, cos_ref, sin_ref,
                n_ref, q_ref, k_ref, v_ref, do_ref, wkv):
    @pl.when(pl.program_id(0) == 0)
    def _():
        wkv[:, :HEAD_DIM] = wk_ref[...]
        wkv[:, HEAD_DIM:] = wv_ref[...]

    xf = x_ref[...].astype(F32)
    inv = lax.rsqrt(jnp.mean(xf * xf, axis=-1, keepdims=True) + NORM_EPS)
    n_ref[...] = (xf * inv * gain_ref[...]).astype(BF16)
    n = n_ref[...]
    q = mm(n, wq_ref[...])
    kv = mm(n, wkv[...])
    d = mm_nt(dout_ref[...], wo_ref[...])
    cos_v, sin_v = tile_angles(cos_ref, sin_ref, pl.program_id(0))
    for h in TWO:
        cols = slice(h * HEAD_DIM, (h + 1) * HEAD_DIM)
        q_ref[h] = rotate(q[:, cols], cos_v, sin_v).astype(BF16)
        do_ref[h] = d[:, cols].astype(BF16)
    k_ref[...] = rotate(kv[:, :HEAD_DIM], cos_v, sin_v).astype(BF16)
    v_ref[...] = kv[:, HEAD_DIM:].astype(BF16)


def proj(kv, x, dout, gain, w_query, w_key, w_value, w_out, cos_t, sin_t):
    row = lambda w: pl.BlockSpec((TILE, w), lambda i, s: (i, 0))
    whole = lambda a, b: pl.BlockSpec((a, b), lambda i, s: (0, 0))
    head2 = pl.BlockSpec((2, TILE, HEAD_DIM), lambda i, s: (0, i, 0))
    wspec = pl.BlockSpec((D_MODEL, HEAD_DIM), lambda i, s: (0, s[0]))
    sds = jax.ShapeDtypeStruct
    return pl.pallas_call(
        proj_kernel,
        grid_spec=pltpu.PrefetchScalarGridSpec(
            num_scalar_prefetch=1, grid=(SEQ // TILE,),
            in_specs=[row(D_MODEL), row(D_MODEL), whole(1, D_MODEL), whole(D_MODEL, 2 * HEAD_DIM), wspec, wspec,
                      whole(2 * HEAD_DIM, D_MODEL)] + [whole(TILE + SEQ // TILE, HEAD_DIM)] * 2,
            out_specs=(row(D_MODEL), head2, row(HEAD_DIM), row(HEAD_DIM), head2),
            scratch_shapes=[pltpu.VMEM((D_MODEL, 2 * HEAD_DIM), BF16)]),
        out_shape=(sds((SEQ, D_MODEL), BF16), sds((2, SEQ, HEAD_DIM), BF16), sds((SEQ, HEAD_DIM), BF16),
                   sds((SEQ, HEAD_DIM), BF16), sds((2, SEQ, HEAD_DIM), BF16)),
        compiler_params=pltpu.CompilerParams(vmem_limit_bytes=56 * MIB),
        cost_estimate=pl.CostEstimate(flops=2 * SEQ * D_MODEL * 768, bytes_accessed=58 * MIB, transcendentals=0),
        name="proj")(kv, x, dout, gain, w_query, w_key, w_value, w_out, cos_t, sin_t)


def attn_kernel(first, nt, dp_ref, q_ref, do_ref, k_ref, v_ref, cos_ref, sin_ref, *refs):
    prev, (o_ref, dq_ref, od_ref, dkv_ref, kt, vt, qt, dot_, qc, dc, s) = refs[:-11], refs[-11:]
    i = pl.program_id(0) + first
    wide = 2 * TILE
    c2 = SCORE_SCALE * math.log2(math.e)

    def keys(b):
        return pl.ds(scaled(b, KEYS), KEYS)

    @pl.when(i == first)
    def _():
        def turn(b, _):
            r = keys(b)
            kt[b] = k_ref[r, :].T
            vt[b] = v_ref[r, :].T
            dkv_ref[r, :] = prev[-1][r, :] if prev else jnp.zeros((KEYS, 2 * HEAD_DIM), F32)
            return 0

        lax.fori_loop(0, SEQ // KEYS, turn, 0)

    for h in TWO:
        r = slice(h * TILE, (h + 1) * TILE)
        qc[r, :] = q_ref[h]
        dc[r, :] = do_ref[h]
        qt[:, r] = q_ref[h].T
        dot_[:, r] = do_ref[h].T

    def fold(f, v):
        a = v[:8]
        for g in range(1, KEYS // 8):
            a = f(a, v[g * 8:(g + 1) * 8])
        return a

    def score(b, m):
        sb = mm(k_ref[keys(b), :], qt[...])
        s[b] = sb
        return jnp.maximum(m, fold(jnp.maximum, sb))

    last = i * TILE // KEYS
    m8 = lax.fori_loop(0, last, score, jnp.full((8, wide), NEG, F32))
    sb = mm(k_ref[keys(last), :], qt[...])
    key = last * KEYS + lax.broadcasted_iota(jnp.int32, (KEYS, wide), 0)
    query = i * TILE + lax.broadcasted_iota(jnp.int32, (KEYS, wide), 1) % TILE
    sb = jnp.where(key <= query, sb, NEG)
    s[last] = sb
    m8 = jnp.maximum(m8, fold(jnp.maximum, sb))
    m = jnp.max(m8, axis=0, keepdims=True) * c2

    def expo(b, l):
        p = jnp.exp2(s[b] * c2 - m)
        s[b] = p
        return l + fold(jnp.add, p)

    l8 = lax.fori_loop(0, last + 1, expo, jnp.zeros((8, wide), F32))
    inv_l = 1.0 / jnp.sum(l8, axis=0, keepdims=True)

    def value(b, acc):
        p = s[b] * inv_l
        s[b] = p
        return acc + mm(vt[b], p.astype(BF16))

    ot = lax.fori_loop(0, last + 1, value, jnp.zeros((HEAD_DIM, wide), F32))
    row_dot = jnp.sum(ot * dot_[...].astype(F32), axis=0, keepdims=True)

    def grads(b, acc):
        p = s[b]
        dp = mm(v_ref[keys(b), :], dot_[...])
        ds = (p * (dp - row_dot)).astype(BF16)
        dkv_ref[keys(b), :HEAD_DIM] += mm(ds, qc[...])
        dkv_ref[keys(b), HEAD_DIM:] += mm(p.astype(BF16), dc[...])
        return acc + mm(kt[b], ds)

    dqt = lax.fori_loop(0, last + 1, grads, jnp.zeros((HEAD_DIM, wide), F32))

    cos_v, sin_v = tile_angles(cos_ref, sin_ref, i)
    for h in TWO:
        cols = slice(h * HEAD_DIM, (h + 1) * HEAD_DIM)
        r = slice(h * TILE, (h + 1) * TILE)
        o = ot[:, r].T.astype(BF16)
        dq = rotate(dqt[:, r].T * SCORE_SCALE, cos_v, -sin_v).astype(BF16)
        o_ref[:, cols] = o
        dq_ref[:, cols] = dq
        place = dp_ref[0] ^ h
        od_ref[place] = o.astype(F32)
        od_ref[2 + place] = dq.astype(F32)

    if prev:
        @pl.when(i == nt - 1)
        def _():
            def finish(b, _):
                r = pl.ds(scaled(b, TILE), TILE)
                cos_b, sin_b = tile_angles(cos_ref, sin_ref, b)
                dkv_ref[r, :HEAD_DIM] = rotate(dkv_ref[r, :HEAD_DIM] * SCORE_SCALE, cos_b, -sin_b)
                return 0

            lax.fori_loop(0, nt, finish, 0)


def attention(dp, q, do, k, v, cos_t, sin_t, first, count, prev):
    n = SEQ // TILE
    head2 = pl.BlockSpec((2, TILE, HEAD_DIM), lambda i, s: (0, i + first, 0))
    whole = pl.BlockSpec((SEQ, HEAD_DIM), lambda i, s: (0, 0))
    angle = pl.BlockSpec((TILE + n, HEAD_DIM), lambda i, s: (0, 0))
    both = pl.BlockSpec((TILE, 2 * HEAD_DIM), lambda i, s: (i + first, 0))
    sums = pl.BlockSpec((SEQ, 2 * HEAD_DIM), lambda i, s: (0, 0))
    sds, vmem = jax.ShapeDtypeStruct, pltpu.VMEM
    heads_t, turned, stacked = vmem((SEQ // KEYS, HEAD_DIM, KEYS), BF16), vmem((HEAD_DIM, 2 * TILE), BF16), vmem((2 * TILE, HEAD_DIM), BF16)
    args = (dp, q, do, k, v, cos_t, sin_t)
    return pl.pallas_call(
        functools.partial(attn_kernel, first, n),
        grid_spec=pltpu.PrefetchScalarGridSpec(
            num_scalar_prefetch=1, grid=(count,),
            in_specs=[head2, head2, whole, whole, angle, angle] + ([pl.BlockSpec(memory_space=pl.ANY)] * 3 + [sums] if prev else []),
            out_specs=(both, both, pl.BlockSpec((4, TILE, HEAD_DIM), lambda i, s: (0, i + first, 0)), sums),
            scratch_shapes=[heads_t, heads_t, turned, turned, stacked, stacked, vmem((SEQ // KEYS, KEYS, 2 * TILE), F32)]),
        out_shape=(sds((SEQ, 2 * HEAD_DIM), BF16), sds((SEQ, 2 * HEAD_DIM), BF16), sds((4, SEQ, HEAD_DIM), F32), sds((SEQ, 2 * HEAD_DIM), F32)),
        input_output_aliases={len(args) + a: a for a in range(len(prev))},
        compiler_params=pltpu.CompilerParams(vmem_limit_bytes=56 * MIB),
        cost_estimate=pl.CostEstimate(flops=6 * 10**9, bytes_accessed=14 * MIB, transcendentals=10**6),
        name="attention")(*args, *prev)


def wgrad_kernel(n_ref, dq_ref, dkv_ref, dkv_c_ref, gq, gk, gv, rhs):
    wide = 2 * HEAD_DIM

    @pl.when(pl.program_id(0) == 0)
    def _():
        rhs[:, :wide] = dq_ref[...]
        rhs[:, wide:] = (dkv_ref[...] + dkv_c_ref[...]).astype(BF16)

    g = lax.dot_general(n_ref[...], rhs[...], TN_DIMS, preferred_element_type=F32)
    gq[...] = g[:, :wide]
    gk[...] = g[:, wide:wide + HEAD_DIM]
    gv[...] = g[:, wide + HEAD_DIM:]


def wgrad(n, dq, dkv, dkv_c):
    tile = WT
    whole = pl.BlockSpec((SEQ, 2 * HEAD_DIM), lambda i: (0, 0))
    out = lambda width: pl.BlockSpec((tile, width), lambda i: (i, 0))
    widths = (2 * HEAD_DIM, HEAD_DIM, HEAD_DIM)
    return pl.pallas_call(
        wgrad_kernel, grid=(D_MODEL // tile,),
        in_specs=[pl.BlockSpec((SEQ, tile), lambda i: (0, i)), whole, whole, whole],
        out_specs=tuple(out(w) for w in widths),
        out_shape=tuple(jax.ShapeDtypeStruct((D_MODEL, w), F32) for w in widths),
        scratch_shapes=[pltpu.VMEM((SEQ, 4 * HEAD_DIM), BF16)],
        compiler_params=pltpu.CompilerParams(vmem_limit_bytes=56 * MIB),
        cost_estimate=pl.CostEstimate(flops=2 * SEQ * D_MODEL * 4 * HEAD_DIM, bytes_accessed=32 * MIB, transcendentals=0),
        name="wgrad")(n, dq, dkv, dkv_c)


def rope_tables():
    lane = jnp.arange(HEAD_DIM)
    inv_freq = ROPE_BASE ** (-(lane - lane % 2).astype(F32) / HEAD_DIM)
    rows = jnp.concatenate([jnp.arange(TILE), jnp.arange(SEQ // TILE) * TILE]).astype(F32)
    angles = rows[:, None] * inv_freq[None, :]
    return jnp.cos(angles), jnp.sin(angles)


def block_fn(hidden, grad_out, norm_gain, w_query, w_key, w_value, w_out):
    seq_len, d_model = hidden.shape[1:]
    x, dout = hidden[0], grad_out[0]
    t = lax.axis_index('tp')
    dp = lax.axis_index('dp')
    j = t % 4
    rows = seq_len // 4
    pre = jnp.stack([dp, j, t // 2]).astype(jnp.int32)
    dpa, kva = pre[0:1], pre[2:3]

    def flip(v, d):
        return lax.ppermute(v, 'tp', [(s, s ^ d) for s in range(16)])

    def over_x(v):
        return lax.ppermute(v, 'dp', [(0, 1), (1, 0)])

    woa, wob = widen(dpa, w_out, 0)
    wo_ya = flip(woa, 2)
    wo_yb = over_x(wo_ya)
    fos = [flip(woa, 1), flip(wob, 1), wo_ya, wo_yb, flip(wo_ya, 1), flip(wo_yb, 1)]
    kva, w_query_, _ = lax.optimization_barrier((kva, w_query, woa))
    cos_t, sin_t = rope_tables()
    gain = norm_gain.astype(F32).reshape(1, d_model)
    n, q, k, v, do = proj(kva, x, dout, gain, w_query_, w_key, w_value, w_out, cos_t, sin_t)
    dpb, _ = lax.optimization_barrier((dpa, k))
    wqa, wqb = widen(dpb, w_query, 1)
    wqs = [flip(wqa, 1), flip(wqb, 1), flip(wqa, 2)]
    dpc, _ = lax.optimization_barrier((dpa, wqa))
    part = attention(dpc, q, do, k, v, cos_t, sin_t, 0, SEQ // TILE // 2, ())
    o, dq, od, dkv_part = attention(dpc, q, do, k, v, cos_t, sin_t, SEQ // TILE // 2, SEQ // TILE // 2, part)

    def rows_of(jj):
        return lax.dynamic_slice(od, (0, jj * rows, 0), (2, rows, HEAD_DIM))

    os = [flip(rows_of(j ^ d), d) for d in (1, 2, 3)]
    dkv_c = flip(dkv_part, 1)
    grad_w_query, gk, gv = wgrad(n, dq, dkv_part, dkv_c)
    o, _ = lax.optimization_barrier((o, gk))
    grad_w_out = jnp.einsum('se,sd->ed', o, dout, preferred_element_type=F32)

    tiles = (seq_len // CR, CR, d_model)
    out, dx, gg = comm(od, os, w_out, fos, dkv_part, dkv_c, w_query, wqs, w_key, w_value,
                               x.reshape(tiles), dout.reshape(tiles), gain)
    return (out.reshape(1, seq_len, d_model), dx.reshape(1, seq_len, d_model), gg.reshape(d_model), grad_w_query, gk, gv, grad_w_out)


def solution(mesh):
    act_spec = P('dp', None, None)

    return jax.shard_map(
        block_fn, mesh=mesh,
        in_specs=(act_spec, act_spec, P(None), P(None, 'tp'), P(None, None), P(None, None), P('tp', None)),
        out_specs=(act_spec, act_spec, P('dp'), P('dp', 'tp'), P('dp', 'tp'), P('dp', 'tp'), P(('dp', 'tp'), None)),
        check_vma=False)
```

```python
import functools
import math
import jax
import jax.numpy as jnp
from jax import lax
from jax.experimental import pallas as pl
from jax.experimental.pallas import tpu as pltpu
from jax.sharding import PartitionSpec as P

F32, BF16 = jnp.float32, jnp.bfloat16
MESH = pl.DeviceIdType.MESH
NORM_EPS = 1.0e-5
MIB = 2 ** 20
TWO, FOUR, SIX = range(2), range(4), range(6)
CR, CC = 8, 2048
GC = 512
D_MODEL = 4096
SHARD = 128
RCH = SHARD // CR
HALVES = D_MODEL // CC
PER = RCH * HALVES
R = 2 * PER
OWN, CSEND, YSEND, CONV = 4, 7, 8, 9
LAG = 3
L, QUICK = R - 1, 2
NI = R + CONV + 1
DP, DR, D, DS = 8, 8, 16, 4
ROWS, HD, TC = 512, 128, 256
TILES = D_MODEL // TC
LATER = 4
UP, DOWN = (3, 2, 1), (0, 1, 2)
T_X, T_D, T_W = 9, 10, 12
NT_DIMS = (((1,), (1,)), ((), ()))
TN_DIMS = (((0,), (0,)), ((), ()))


def inside(r, n):
    return (r >= 0) & (r < n)


def scaled(a, unit):
    return pl.multiple_of(a * unit, unit)


def comm_kernel(od, od5, oc, oy, oyc, wo, foca, focb, foya, foyb, foza, fozb,
                dkv, dkv_c, wq, wca, wcb, wya, wk, wv, x_hbm, dout_hbm, gain_ref,
                out0, out1, gain_out, wyb, wza, wzb,
                pbuf, upb, dnb, zb, yb, cz, cy, fb, xo, do, stage, gacc,
                la, wof, wob, ra, p0, dqo, dqr, kva, kvs, kvr, lhs, wtf, wtq, wtk, rd, p1,
                psem, up_r, dn_r, z_r, y_r, c_r,
                up_s, dn_s, zu_s, zd_s, za_s, y_s, c_s, o_sem, l_sem, e_s, e_r, w_sem, wo_sem):
    dp = lax.axis_index("dp")
    t = lax.axis_index("tp")
    z, y, c = t // 4, (t // 2) % 2, t % 2
    j = t % 4

    def dev(zz, yy, cc):
        return (dp, zz * 4 + yy * 2 + cc)

    above, below = dev(lax.rem(z + 1, 4), y, c), dev(lax.rem(z + 3, 4), y, c)

    def remote(src, dst, ss, rs, device):
        return pltpu.make_async_remote_copy(src_ref=src, dst_ref=dst, send_sem=ss, recv_sem=rs,
                                            device_id=device, device_id_type=MESH)

    def rowcol(r):
        kk = lax.rem(r, PER)
        first = r < PER
        row = jnp.where(first, lax.rem(kk, RCH), kk // HALVES)
        half = jnp.where(first, kk // RCH, lax.rem(kk, HALVES))
        return row, scaled(half, CC)

    def p_copy(p, r):
        rr, cc = rowcol(r)
        return pltpu.make_async_copy(p.at[:, rr, :, pl.ds(cc, CC)], pbuf.at[lax.rem(r, DP)], psem.at[lax.rem(r, DP)])

    def p_start(r):
        @pl.when(r < PER)
        def _():
            p_copy(p0, r).start()

        @pl.when((r >= PER) & (r < R))
        def _():
            p_copy(p1, r).start()

    def line_copy(buf, src, r, o, i, ss, rs, device):
        s = lax.rem(r, DR)
        return remote(pbuf.at[lax.rem(r, DP), o] if src is None else src.at[s, o], buf.at[s, o], ss.at[o, lax.rem(i, DS)], rs.at[o, s], device)

    def up_copy(r, o, i, src=upb):
        return line_copy(upb, src, r, o, i, up_s, up_r, above)

    def dn_copy(r, o, i, src=dnb):
        return line_copy(dnb, src, r, o, i, dn_s, dn_r, below)

    def cut(ref, small):
        return ref.at[:, pl.ds(0, GC)] if small else ref

    def along_z(r, q, i, small, sem, device):
        v = cut(zb.at[lax.rem(r, D), q], small)
        return remote(v, v, sem.at[lax.rem(i, DS)], z_r.at[q, lax.rem(r, D)], device)

    def y_copy(r, q, i, small, late):
        s = lax.rem(r, D)
        return remote(cut(zb.at[s, q], small), cut(yb.at[s, q], small), y_s.at[late, q, lax.rem(i, DS)], y_r.at[q, s], dev(z, 1 - y, c))

    def c_copy(k, r, i, small, late):
        s = lax.rem(r, D)
        src, dst = ((zb, cz), (yb, cy))[k]
        src, dst = src.at[s], dst.at[s]
        if small:
            src, dst = src.at[:, :, pl.ds(0, GC)], dst.at[:, :, pl.ds(0, GC)]
        return remote(src, dst, c_s.at[late, k, lax.rem(i, DS)], c_r.at[k, s], dev(z, y, 1 - c))

    def sized(i, delay, quick, f):
        @pl.when(inside(i - delay, L))
        def _():
            f(i - delay, False, 0)

        for small in (False, True):
            @pl.when(i - quick == L + small)
            def _():
                f(i - quick, small, 1)

    bufs = (zb, yb, cz, cy)

    def src_j(k):
        yy = y if k in (0, 2) else 1 - y
        cc = c if k in (0, 1) else 1 - c
        return yy * 2 + cc

    def o_copy(out, r, b, k):
        rr, cc = rowcol(r)
        return pltpu.make_async_copy(stage.at[b, k], out.at[src_j(k), :, rr, :, pl.ds(cc, CC)], o_sem.at[b, k])

    def when_line(i, hop, order, mine, make, f):
        r = i - hop
        for o in order:
            @pl.when(inside(r, R) & mine(o))
            def _():
                @pl.when(hop == 0)
                def _():
                    f(make(r, o, i, None))

                @pl.when(hop > 0)
                def _():
                    f(make(r, o, i))

    def when_sums(i, f):
        when_line(i, z, UP, lambda o: z < o, up_copy, f)
        when_line(i, 3 - z, DOWN, lambda o: z > o, dn_copy, f)

    def gathered_at(q):
        h = jnp.abs(z - q)
        return OWN + h, OWN + jnp.minimum(h, 1)

    def when_ag(i, q, f):
        def sends(r, small, late):
            if late:
                @pl.when(z == q)
                def _():
                    for d in UP:
                        f(along_z(r, q, i, small, za_s.at[d - 1], dev(lax.rem(z + d, 4), y, c)))
            else:
                @pl.when((z >= q) & (z < 3))
                def _():
                    f(along_z(r, q, i, small, zu_s.at[q], above))

                @pl.when((z <= q) & (z > 0))
                def _():
                    f(along_z(r, q, i, small, zd_s.at[q], below))

            f(y_copy(r, q, i, small, late))

        sized(i, *gathered_at(q), sends)

    def when_c(i, f):
        for k, at in enumerate((CSEND, YSEND)):
            sized(i, at, at - QUICK, lambda r, small, late: f(c_copy(k, r, i, small, late)))

    def head_at(p):
        return pl.ds(scaled(dp ^ p, HD), HD)

    def rows_of(jj):
        return pl.ds(scaled(jj, ROWS), ROWS)

    def wo_loads(n):
        b = lax.rem(n, 2)
        cols = pl.ds(scaled(n, TC), TC)
        cps = [(src.at[:, cols], wof.at[b, k]) for k, src in enumerate((foca, focb, foya, foyb, foza, fozb))] + [(wo.at[:, cols], wob.at[b])]
        return [pltpu.make_async_copy(a, v, wo_sem.at[b, k]) for k, (a, v) in enumerate(cps)]

    def first_tile(n):
        b = lax.rem(n, 2)
        for cp in wo_loads(n):
            cp.wait()
        for p in TWO:
            ra[p * HD:(p + 1) * HD, :] = wob[b, head_at(p), :]
        for k in SIX:
            ra[(2 + k) * HD:(3 + k) * HD, :] = wof[b, k].astype(BF16)
        tile = jnp.dot(la[...], ra[...], preferred_element_type=F32)
        p0[:, :, :, pl.ds(scaled(n, TC), TC)] = tile.reshape(4, RCH, CR, TC)

    def dq_send(d):
        return remote(od.at[pl.ds(2, 2), rows_of(j ^ d)], dqr.at[d - 1], e_s.at[d - 1], e_r.at[d - 1], (dp, t ^ d))

    exchange = [dq_send(1), dq_send(2), dq_send(3),
                remote(kvs.at[0], kvr, e_s.at[3], e_r.at[3], (dp, t ^ 2)),
                remote(wya, wyb, e_s.at[4], e_r.at[4], (1 - dp, t)),
                remote(wya, wza, e_s.at[5], e_r.at[5], (dp, t ^ 1))]
    last = remote(wyb, wzb, e_s.at[6], e_r.at[6], (dp, t ^ 1))
    own = pltpu.make_async_copy(od.at[pl.ds(2, 2), rows_of(j)], dqo, l_sem.at[2])

    def kv_loads(m):
        rows = rows_of(j ^ 2 ^ m)
        return [pltpu.make_async_copy(src.at[rows], kva.at[k], l_sem.at[3 + k]) for k, src in enumerate((dkv, dkv_c))]

    def kv_sum(m, out):
        for cp in kv_loads(m):
            cp.wait()
        kvs[out] = kva[0] + kva[1]

    kv_own = t // 2

    def tile_loads(n):
        b = lax.rem(n, 2)
        r = pl.ds(scaled(n, TC), TC)
        cps = [(src.at[r], wtf.at[b, k]) for k, src in enumerate((wca, wcb, wya, wyb, wza, wzb))] + [(wq.at[r], wtq.at[b])]
        cps += [(src.at[r, pl.ds(scaled(h, HD), HD)], wtk.at[b, k])
                for k, (src, h) in enumerate(((wk, kv_own), (wv, kv_own), (wk, kv_own ^ 1), (wv, kv_own ^ 1)))]
        return [pltpu.make_async_copy(a, v, w_sem.at[b, k]) for k, (a, v) in enumerate(cps)]

    def second_tile(n):
        b = lax.rem(n, 2)
        for cp in tile_loads(n):
            cp.wait()
        for p in TWO:
            rd[:, p * HD:(p + 1) * HD] = wtq[b, :, head_at(p)]
        for k in SIX:
            rd[:, (2 + k) * HD:(3 + k) * HD] = wtf[b, k].astype(BF16)
        for k in FOUR:
            rd[:, (8 + k) * HD:(9 + k) * HD] = wtk[b, k]
        tile = lax.dot_general(lhs[...], rd[...], NT_DIMS, preferred_element_type=F32)
        p1[:, :, :, pl.ds(scaled(n, TC), TC)] = tile.reshape(4, RCH, CR, TC)

    base = (j * 4 + z) * RCH
    owned = [pltpu.make_async_copy(x_hbm.at[pl.ds(base, RCH)], xo, l_sem.at[0]),
             pltpu.make_async_copy(dout_hbm.at[pl.ds(base, RCH)], do, l_sem.at[1])]

    def products(i):
        for at in TWO:
            @pl.when(i == at + 1)
            def _():
                kv_sum(2 * at, at)
                if at == 0:
                    for cp in kv_loads(2):
                        cp.start()

        @pl.when(i == 2)
        def _():
            exchange[3].start()
            for cp in owned:
                cp.wait()

        n = i + TILES // 2 - LATER

        @pl.when((i >= LATER) & (n + 1 < TILES))
        def _():
            for cp in wo_loads(n + 1):
                cp.start()

        @pl.when((i >= LATER) & (n < TILES))
        def _():
            first_tile(n)

        @pl.when(i == T_X)
        def _():
            exchange[4].wait()
            last.start()

        @pl.when(i == T_D)
        def _():
            for cp in [own] + exchange[:4] + exchange[5:]:
                cp.wait()
            for p in TWO:
                lhs[:, p * HD:(p + 1) * HD] = dqo[p].astype(BF16)
                for k in range(3):
                    lhs[:, (2 * k + 2 + p) * HD:(2 * k + 3 + p) * HD] = dqr[k, p].astype(BF16)
            lhs[:, 8 * HD:10 * HD] = kvs[1].astype(BF16)
            lhs[:, 10 * HD:] = kvr[...].astype(BF16)

        @pl.when(i == T_W)
        def _():
            last.wait()

        @pl.when(inside(i - T_W, TILES))
        def _():
            for cp in tile_loads(i - T_W):
                cp.start()

        @pl.when(inside(i - T_W - 1, TILES))
        def _():
            second_tile(i - T_W - 1)

    for cp in exchange[:3] + exchange[4:] + [own] + kv_loads(0):
        cp.start()
    loads = [pltpu.make_async_copy(src.at[p], p0.at[:, :, :, pl.ds((2 * k + p) * HD, HD)], l_sem.at[5 + 2 * k + p])
              for k, src in enumerate((od5.at[:, pl.ds(j * 4, 4)], oc, oy, oyc)) for p in TWO]
    for cp in loads + wo_loads(0) + owned:
        cp.start()
    gacc[...] = jnp.zeros_like(gacc)
    for cp in loads:
        cp.wait()
    for k in FOUR:
        for p in TWO:
            at = slice((2 * k + p) * HD, (2 * k + p + 1) * HD)
            la[:, at] = p0[:, :, :, at].reshape(ROWS, HD).astype(BF16)

    def first_half(n, _):
        for cp in wo_loads(n + 1):
            cp.start()
        first_tile(n)
        return 0

    lax.fori_loop(0, TILES // 2, first_half, 0)
    p_start(0)
    p_start(1)

    def body(i, _):
        products(i)

        ip = i - LAG

        @pl.when(ip >= 0)
        def _():
            when_sums(ip, lambda cp: cp.wait_send())
            for q in FOUR:
                when_ag(ip, q, lambda cp: cp.wait_send())
            when_c(ip, lambda cp: cp.wait_send())

        p_start(i + 2)

        @pl.when(i < R)
        def _():
            p_copy(p0, i).wait()

        def take(r, hop, order, make, buf, past):
            @pl.when(inside(r, R) & (hop > 0))
            def _():
                for o in order:
                    @pl.when(past(o))
                    def _():
                        make(r, o, i).wait_recv()
                        buf[lax.rem(r, DR), o] += pbuf[lax.rem(r, DP), o]

        take(i - z, z, UP, up_copy, upb, lambda o: z < o)
        take(i - 3 + z, 3 - z, DOWN, dn_copy, dnb, lambda o: z > o)

        rf = i - 3
        fs = lax.rem(rf, 2)

        @pl.when(inside(rf, R))
        def _():
            fb[fs] = pbuf[lax.rem(rf, DP), z]

            @pl.when(z > 0)
            def _():
                up_copy(rf, z, i).wait_recv()
                fb[fs] += upb[lax.rem(rf, DR), z]

            @pl.when(z < 3)
            def _():
                dn_copy(rf, z, i).wait_recv()
                fb[fs] += dnb[lax.rem(rf, DR), z]

            rr, cc = rowcol(rf)

            @pl.when(rf < PER)
            def _():
                zb[lax.rem(rf, D), z] = (xo[rr, :, pl.ds(cc, CC)].astype(F32) + fb[fs]).astype(BF16).astype(F32)

            @pl.when((rf >= PER) & (fs == 1))
            def _():
                xr = xo[rr].astype(F32)
                inv = lax.rsqrt(jnp.mean(xr * xr, axis=-1, keepdims=True) + NORM_EPS)
                u = xr * inv
                dn = jnp.concatenate([fb[0], fb[1]], axis=1)
                gg = dn * gain_ref[...]
                m = jnp.mean(gg * u, axis=-1, keepdims=True)
                dx = (do[rr].astype(F32) + inv * (gg - u * m)).astype(BF16).astype(F32)
                gacc[...] += dn * u
                zb[lax.rem(rf - 1, D), z] = dx[:, :CC]
                zb[lax.rem(rf, D), z] = dx[:, CC:]

        @pl.when(rf == R)
        def _():
            total = jnp.sum(gacc[...], axis=0, keepdims=True)
            zb[R % D, z, :, :GC] = jnp.concatenate([total[:, a * GC:(a + 1) * GC] for a in range(CR)], axis=0)

        when_sums(i, lambda cp: cp.start())

        for q in FOUR:
            @pl.when(z != q)
            def _():
                sized(i, *gathered_at(q), lambda r, small, late: along_z(r, q, i, small, zu_s.at[q], above).wait_recv())

            when_ag(i, q, lambda cp: cp.start())

        for q in FOUR:
            sized(i, YSEND, YSEND - QUICK, lambda r, small, late: y_copy(r, q, i, small, late).wait_recv())

        when_c(i, lambda cp: cp.start())

        def stored(i, f):
            r = i - CONV

            @pl.when(inside(r, PER))
            def _():
                f(out0, r, lax.rem(i, 2))

            @pl.when((r >= PER) & (r < L))
            def _():
                f(out1, r, lax.rem(i, 2))

            @pl.when(r + QUICK == L)
            def _():
                f(out1, L, 2)

        def wait_stored(out, r, b):
            for k in FOUR:
                o_copy(out, r, b, k).wait()

        def store(out, r, b):
            for k in FOUR:
                for q in FOUR:
                    stage[b, k, q] = bufs[k][lax.rem(r, D), q].astype(BF16)
                o_copy(out, r, b, k).start()

        stored(i - 2, wait_stored)
        for k in TWO:
            sized(i, CONV, CONV - QUICK, lambda r, small, late: c_copy(k, r, i, small, late).wait_recv())
        stored(i, store)

        @pl.when(i == R + CONV - QUICK)
        def _():
            acc = jnp.zeros((CR, GC), F32)
            for k in FOUR:
                for q in FOUR:
                    acc = acc + bufs[k][R % D, q, :, :GC]
            for h in range(CR):
                for a in range(GC // HD):
                    gain_out[h * (GC // HD) + a] = acc[h, a * HD:(a + 1) * HD]

        return 0

    lax.fori_loop(0, NI, body, 0)


def comm(od, os, wo, fos, dkv, dkv_c, wq, wqs, wk, wv, x, dout, gain):
    anyspec = pl.BlockSpec(memory_space=pl.ANY)
    hbm = pl.BlockSpec(memory_space=pltpu.HBM)
    vm = pl.BlockSpec(memory_space=pltpu.VMEM)
    dma, vmem, sds = pltpu.SemaphoreType.DMA, pltpu.VMEM, jax.ShapeDtypeStruct
    ch = (CR, CC)
    full = sds((4, 4, RCH, CR, D_MODEL), BF16)
    land = sds((D_MODEL, HD), F32)
    part = vmem((4, RCH, CR, D_MODEL), F32)
    owned = vmem((RCH, CR, D_MODEL), BF16)
    gathered = vmem((D, 4) + ch, F32)
    line = vmem((DR, 4) + ch, F32)
    pair = vmem((2, ROWS, 2 * HD), F32)
    return pl.pallas_call(
        comm_kernel,
        out_shape=(full, full, sds((D_MODEL // HD, HD), F32)) + (land,) * 3,
        in_specs=[hbm] * 22 + [vm],
        out_specs=(anyspec, anyspec, vm) + (hbm,) * 3,
        scratch_shapes=[
            vmem((DP, 4) + ch, F32), line, line, gathered, gathered, gathered, gathered, vmem((2,) + ch, F32),
            owned, owned, vmem((3, 4, 4) + ch, BF16), vmem((CR, D_MODEL), F32),
            vmem((ROWS, 8 * HD), BF16), vmem((2, 6, HD, TC), F32), vmem((2, 2 * HD, TC), BF16),
            vmem((8 * HD, TC), BF16), part,
            vmem((2, ROWS, HD), F32), vmem((3, 2, ROWS, HD), F32), pair, pair, vmem((ROWS, 2 * HD), F32),
            vmem((ROWS, 12 * HD), BF16), vmem((2, 6, TC, HD), F32), vmem((2, TC, 2 * HD), BF16), vmem((2, 4, TC, HD), BF16),
            vmem((TC, 12 * HD), BF16), part,
            dma((DP,)), dma((4, DR)), dma((4, DR)), dma((4, D)), dma((4, D)), dma((2, D)),
            *[dma((4, DS))] * 5, dma((2, 4, DS)), dma((2, 2, DS)), dma((3, 4)), dma((13,)),
            dma((7,)), dma((7,)), dma((2, 11)), dma((2, 7)),
        ],
        compiler_params=pltpu.CompilerParams(has_side_effects=True, vmem_limit_bytes=62 * MIB),
        cost_estimate=pl.CostEstimate(flops=13 * 10**9, bytes_accessed=10**8, transcendentals=0),
        name="comm",
    )(od, od.reshape(4, 16, RCH, CR, HD), *[o.reshape(2, 4, RCH, CR, HD) for o in os], wo, *fos, dkv, dkv_c, wq, *wqs, wk, wv, x, dout, gain)[:3]


HEAD_DIM = 128
ROPE_BASE = 10000.0
SCORE_SCALE = 1.0 / math.sqrt(HEAD_DIM)
SEQ = 2048
WT = 512
NEG = -1.0e30 / SCORE_SCALE
TILE, KEYS = 256, 512


def mm(a, b):
    return jnp.dot(a, b, preferred_element_type=F32)


def mm_nt(a, b):
    return lax.dot_general(a, b, NT_DIMS, preferred_element_type=F32)


def widen_kernel(axis, dp_ref, w_ref, *outs):
    for p, out in enumerate(outs):
        at = pl.ds(scaled(dp_ref[0] ^ p, HEAD_DIM), HEAD_DIM)
        out[...] = (w_ref[:, at] if axis else w_ref[at, :]).astype(F32)


def widen(dp, w, axis):
    tile = 2048
    shape = lambda width: (tile, width) if axis else (width, tile)
    index = (lambda i, s: (i, 0)) if axis else (lambda i, s: (0, i))
    half = jax.ShapeDtypeStruct((D_MODEL, HEAD_DIM) if axis else (HEAD_DIM, D_MODEL), F32)
    return pl.pallas_call(
        functools.partial(widen_kernel, axis),
        grid_spec=pltpu.PrefetchScalarGridSpec(
            num_scalar_prefetch=1, grid=(D_MODEL // tile,),
            in_specs=[pl.BlockSpec(shape(2 * HEAD_DIM), index)],
            out_specs=(pl.BlockSpec(shape(HEAD_DIM), index),) * len(TWO)),
        out_shape=(half,) * len(TWO),
        cost_estimate=pl.CostEstimate(flops=10**9, bytes_accessed=6 * MIB, transcendentals=0),
        name="widen")(dp, w)


def swap_pairs(v):
    lane = lax.broadcasted_iota(jnp.int32, v.shape, 1)
    return jnp.where(lane % 2 == 0, pltpu.roll(v, HEAD_DIM - 1, 1), pltpu.roll(v, 1, 1))


def rotate(v, cos_v, sin_v):
    return v * cos_v + swap_pairs(v) * sin_v


def tile_angles(cos_ref, sin_ref, i):
    at = pl.ds(TILE + i, 1)
    ca, sa = cos_ref[at, :], sin_ref[at, :]
    cb, sb = cos_ref[:TILE, :], sin_ref[:TILE, :]
    even = lax.broadcasted_iota(jnp.int32, (TILE, HEAD_DIM), 1) % 2 == 0
    s = sa * cb + ca * sb
    return ca * cb - sa * sb, jnp.where(even, -s, s)


def proj_kernel(kv_ref, x_ref, dout_ref, gain_ref, wq_ref, wk_ref, wv_ref, wo_ref, cos_ref, sin_ref,
                n_ref, q_ref, k_ref, v_ref, do_ref, wkv):
    @pl.when(pl.program_id(0) == 0)
    def _():
        wkv[:, :HEAD_DIM] = wk_ref[...]
        wkv[:, HEAD_DIM:] = wv_ref[...]

    xf = x_ref[...].astype(F32)
    inv = lax.rsqrt(jnp.mean(xf * xf, axis=-1, keepdims=True) + NORM_EPS)
    n_ref[...] = (xf * inv * gain_ref[...]).astype(BF16)
    n = n_ref[...]
    q = mm(n, wq_ref[...])
    kv = mm(n, wkv[...])
    d = mm_nt(dout_ref[...], wo_ref[...])
    cos_v, sin_v = tile_angles(cos_ref, sin_ref, pl.program_id(0))
    for h in TWO:
        cols = slice(h * HEAD_DIM, (h + 1) * HEAD_DIM)
        q_ref[h] = rotate(q[:, cols], cos_v, sin_v).astype(BF16)
        do_ref[h] = d[:, cols].astype(BF16)
    k_ref[...] = rotate(kv[:, :HEAD_DIM], cos_v, sin_v).astype(BF16)
    v_ref[...] = kv[:, HEAD_DIM:].astype(BF16)


def proj(kv, x, dout, gain, w_query, w_key, w_value, w_out, cos_t, sin_t):
    row = lambda w: pl.BlockSpec((TILE, w), lambda i, s: (i, 0))
    whole = lambda a, b: pl.BlockSpec((a, b), lambda i, s: (0, 0))
    head2 = pl.BlockSpec((2, TILE, HEAD_DIM), lambda i, s: (0, i, 0))
    wspec = pl.BlockSpec((D_MODEL, HEAD_DIM), lambda i, s: (0, s[0]))
    sds = jax.ShapeDtypeStruct
    return pl.pallas_call(
        proj_kernel,
        grid_spec=pltpu.PrefetchScalarGridSpec(
            num_scalar_prefetch=1, grid=(SEQ // TILE,),
            in_specs=[row(D_MODEL), row(D_MODEL), whole(1, D_MODEL), whole(D_MODEL, 2 * HEAD_DIM), wspec, wspec,
                      whole(2 * HEAD_DIM, D_MODEL)] + [whole(TILE + SEQ // TILE, HEAD_DIM)] * 2,
            out_specs=(row(D_MODEL), head2, row(HEAD_DIM), row(HEAD_DIM), head2),
            scratch_shapes=[pltpu.VMEM((D_MODEL, 2 * HEAD_DIM), BF16)]),
        out_shape=(sds((SEQ, D_MODEL), BF16), sds((2, SEQ, HEAD_DIM), BF16), sds((SEQ, HEAD_DIM), BF16),
                   sds((SEQ, HEAD_DIM), BF16), sds((2, SEQ, HEAD_DIM), BF16)),
        compiler_params=pltpu.CompilerParams(vmem_limit_bytes=56 * MIB),
        cost_estimate=pl.CostEstimate(flops=2 * SEQ * D_MODEL * 768, bytes_accessed=58 * MIB, transcendentals=0),
        name="proj")(kv, x, dout, gain, w_query, w_key, w_value, w_out, cos_t, sin_t)


def attn_kernel(first, nt, dp_ref, q_ref, do_ref, k_ref, v_ref, cos_ref, sin_ref, *refs):
    prev, (o_ref, dq_ref, od_ref, dkv_ref, kt, vt, qt, dot_, qc, dc, s, g) = refs[:-12], refs[-12:]
    i = pl.program_id(0) + first
    wide = 2 * TILE
    c2 = SCORE_SCALE * math.log2(math.e)

    def keys(b):
        return pl.ds(scaled(b, KEYS), KEYS)

    @pl.when(i == first)
    def _():
        def turn(b, _):
            r = keys(b)
            kt[b] = k_ref[r, :].T
            vt[b] = v_ref[r, :].T
            dkv_ref[r, :] = prev[-1][r, :] if prev else jnp.zeros((KEYS, 2 * HEAD_DIM), F32)
            return 0

        lax.fori_loop(0, SEQ // KEYS, turn, 0)

    for h in TWO:
        r = slice(h * TILE, (h + 1) * TILE)
        qc[r, :] = q_ref[h]
        dc[r, :] = do_ref[h]
        qt[:, r] = q_ref[h].T
        dot_[:, r] = do_ref[h].T

    def fold(f, v):
        a = v[:8]
        for g in range(1, KEYS // 8):
            a = f(a, v[g * 8:(g + 1) * 8])
        return a

    def score(b, m):
        sb = mm(k_ref[keys(b), :], qt[...])
        s[b] = sb
        return jnp.maximum(m, fold(jnp.maximum, sb))

    last = i * TILE // KEYS
    m8 = lax.fori_loop(0, last, score, jnp.full((8, wide), NEG, F32))
    sb = mm(k_ref[keys(last), :], qt[...])
    key = last * KEYS + lax.broadcasted_iota(jnp.int32, (KEYS, wide), 0)
    query = i * TILE + lax.broadcasted_iota(jnp.int32, (KEYS, wide), 1) % TILE
    sb = jnp.where(key <= query, sb, NEG)
    s[last] = sb
    m8 = jnp.maximum(m8, fold(jnp.maximum, sb))
    m = jnp.max(m8, axis=0, keepdims=True) * c2

    def expo(b, l):
        p = jnp.exp2(s[b] * c2 - m)
        s[b] = p
        return l + fold(jnp.add, p)

    l8 = lax.fori_loop(0, last + 1, expo, jnp.zeros((8, wide), F32))
    inv_l = 1.0 / jnp.sum(l8, axis=0, keepdims=True)

    def value(b, carry):
        d, acc = carry
        p = s[b] * inv_l
        dp = mm(v_ref[keys(b), :], dot_[...])
        s[b] = p
        g[b] = dp
        return d + fold(jnp.add, p * dp), acc + mm(vt[b], p.astype(BF16))

    d8, ot = lax.fori_loop(0, last + 1, value, (jnp.zeros((8, wide), F32), jnp.zeros((HEAD_DIM, wide), F32)))
    row_dot = jnp.sum(d8, axis=0, keepdims=True)

    def grads(b, acc):
        p = s[b]
        ds = (p * (g[b] - row_dot)).astype(BF16)
        dkv_ref[keys(b), :HEAD_DIM] += mm(ds, qc[...])
        dkv_ref[keys(b), HEAD_DIM:] += mm(p.astype(BF16), dc[...])
        return acc + mm(kt[b], ds)

    dqt = lax.fori_loop(0, last + 1, grads, jnp.zeros((HEAD_DIM, wide), F32))

    cos_v, sin_v = tile_angles(cos_ref, sin_ref, i)
    for h in TWO:
        cols = slice(h * HEAD_DIM, (h + 1) * HEAD_DIM)
        r = slice(h * TILE, (h + 1) * TILE)
        o = ot[:, r].T.astype(BF16)
        dq = rotate(dqt[:, r].T * SCORE_SCALE, cos_v, -sin_v).astype(BF16)
        o_ref[:, cols] = o
        dq_ref[:, cols] = dq
        place = dp_ref[0] ^ h
        od_ref[place] = o.astype(F32)
        od_ref[2 + place] = dq.astype(F32)

    if prev:
        @pl.when(i == nt - 1)
        def _():
            def finish(b, _):
                r = pl.ds(scaled(b, TILE), TILE)
                cos_b, sin_b = tile_angles(cos_ref, sin_ref, b)
                dkv_ref[r, :HEAD_DIM] = rotate(dkv_ref[r, :HEAD_DIM] * SCORE_SCALE, cos_b, -sin_b)
                return 0

            lax.fori_loop(0, nt, finish, 0)


def attention(dp, q, do, k, v, cos_t, sin_t, first, count, prev):
    n = SEQ // TILE
    head2 = pl.BlockSpec((2, TILE, HEAD_DIM), lambda i, s: (0, i + first, 0))
    whole = pl.BlockSpec((SEQ, HEAD_DIM), lambda i, s: (0, 0))
    angle = pl.BlockSpec((TILE + n, HEAD_DIM), lambda i, s: (0, 0))
    both = pl.BlockSpec((TILE, 2 * HEAD_DIM), lambda i, s: (i + first, 0))
    sums = pl.BlockSpec((SEQ, 2 * HEAD_DIM), lambda i, s: (0, 0))
    sds, vmem = jax.ShapeDtypeStruct, pltpu.VMEM
    heads_t, turned, stacked = vmem((SEQ // KEYS, HEAD_DIM, KEYS), BF16), vmem((HEAD_DIM, 2 * TILE), BF16), vmem((2 * TILE, HEAD_DIM), BF16)
    rows = vmem((SEQ // KEYS, KEYS, 2 * TILE), F32)
    args = (dp, q, do, k, v, cos_t, sin_t)
    return pl.pallas_call(
        functools.partial(attn_kernel, first, n),
        grid_spec=pltpu.PrefetchScalarGridSpec(
            num_scalar_prefetch=1, grid=(count,),
            in_specs=[head2, head2, whole, whole, angle, angle] + ([pl.BlockSpec(memory_space=pl.ANY)] * 3 + [sums] if prev else []),
            out_specs=(both, both, pl.BlockSpec((4, TILE, HEAD_DIM), lambda i, s: (0, i + first, 0)), sums),
            scratch_shapes=[heads_t, heads_t, turned, turned, stacked, stacked, rows, rows]),
        out_shape=(sds((SEQ, 2 * HEAD_DIM), BF16), sds((SEQ, 2 * HEAD_DIM), BF16), sds((4, SEQ, HEAD_DIM), F32), sds((SEQ, 2 * HEAD_DIM), F32)),
        input_output_aliases={len(args) + a: a for a in range(len(prev))},
        compiler_params=pltpu.CompilerParams(vmem_limit_bytes=56 * MIB),
        cost_estimate=pl.CostEstimate(flops=6 * 10**9, bytes_accessed=14 * MIB, transcendentals=10**6),
        name="attention")(*args, *prev)


def wgrad_kernel(n_ref, dq_ref, dkv_ref, dkv_c_ref, gq, gk, gv, rhs):
    wide = 2 * HEAD_DIM

    @pl.when(pl.program_id(0) == 0)
    def _():
        rhs[:, :wide] = dq_ref[...]
        rhs[:, wide:] = (dkv_ref[...] + dkv_c_ref[...]).astype(BF16)

    g = lax.dot_general(n_ref[...], rhs[...], TN_DIMS, preferred_element_type=F32)
    gq[...] = g[:, :wide]
    gk[...] = g[:, wide:wide + HEAD_DIM]
    gv[...] = g[:, wide + HEAD_DIM:]


def wgrad(n, dq, dkv, dkv_c):
    tile = WT
    whole = pl.BlockSpec((SEQ, 2 * HEAD_DIM), lambda i: (0, 0))
    out = lambda width: pl.BlockSpec((tile, width), lambda i: (i, 0))
    widths = (2 * HEAD_DIM, HEAD_DIM, HEAD_DIM)
    return pl.pallas_call(
        wgrad_kernel, grid=(D_MODEL // tile,),
        in_specs=[pl.BlockSpec((SEQ, tile), lambda i: (0, i)), whole, whole, whole],
        out_specs=tuple(out(w) for w in widths),
        out_shape=tuple(jax.ShapeDtypeStruct((D_MODEL, w), F32) for w in widths),
        scratch_shapes=[pltpu.VMEM((SEQ, 4 * HEAD_DIM), BF16)],
        compiler_params=pltpu.CompilerParams(vmem_limit_bytes=56 * MIB),
        cost_estimate=pl.CostEstimate(flops=2 * SEQ * D_MODEL * 4 * HEAD_DIM, bytes_accessed=32 * MIB, transcendentals=0),
        name="wgrad")(n, dq, dkv, dkv_c)


def rope_tables():
    lane = jnp.arange(HEAD_DIM)
    inv_freq = ROPE_BASE ** (-(lane - lane % 2).astype(F32) / HEAD_DIM)
    rows = jnp.concatenate([jnp.arange(TILE), jnp.arange(SEQ // TILE) * TILE]).astype(F32)
    angles = rows[:, None] * inv_freq[None, :]
    return jnp.cos(angles), jnp.sin(angles)


def block_fn(hidden, grad_out, norm_gain, w_query, w_key, w_value, w_out):
    seq_len, d_model = hidden.shape[1:]
    x, dout = hidden[0], grad_out[0]
    t = lax.axis_index('tp')
    dp = lax.axis_index('dp')
    j = t % 4
    rows = seq_len // 4
    pre = jnp.stack([dp, j, t // 2]).astype(jnp.int32)
    dpa, kva = pre[0:1], pre[2:3]

    def flip(v, d):
        return lax.ppermute(v, 'tp', [(s, s ^ d) for s in range(16)])

    def over_x(v):
        return lax.ppermute(v, 'dp', [(0, 1), (1, 0)])

    woa, wob = widen(dpa, w_out, 0)
    wo_ya = flip(woa, 2)
    wo_yb = over_x(wo_ya)
    fos = [flip(woa, 1), flip(wob, 1), wo_ya, wo_yb, flip(wo_ya, 1), flip(wo_yb, 1)]
    kva, w_query_, _ = lax.optimization_barrier((kva, w_query, woa))
    cos_t, sin_t = rope_tables()
    gain = norm_gain.astype(F32).reshape(1, d_model)
    n, q, k, v, do = proj(kva, x, dout, gain, w_query_, w_key, w_value, w_out, cos_t, sin_t)
    dpb, _ = lax.optimization_barrier((dpa, k))
    wqa, wqb = widen(dpb, w_query, 1)
    wqs = [flip(wqa, 1), flip(wqb, 1), flip(wqa, 2)]
    dpc, _ = lax.optimization_barrier((dpa, wqa))
    part = attention(dpc, q, do, k, v, cos_t, sin_t, 0, SEQ // TILE // 2, ())
    o, dq, od, dkv_part = attention(dpc, q, do, k, v, cos_t, sin_t, SEQ // TILE // 2, SEQ // TILE // 2, part)

    def rows_of(jj):
        return lax.dynamic_slice(od, (0, jj * rows, 0), (2, rows, HEAD_DIM))

    os = [flip(rows_of(j ^ d), d) for d in (1, 2, 3)]
    dkv_c = flip(dkv_part, 1)
    grad_w_query, gk, gv = wgrad(n, dq, dkv_part, dkv_c)
    o, _ = lax.optimization_barrier((o, gk))
    grad_w_out = jnp.einsum('se,sd->ed', o, dout, preferred_element_type=F32)

    tiles = (seq_len // CR, CR, d_model)
    out, dx, gg = comm(od, os, w_out, fos, dkv_part, dkv_c, w_query, wqs, w_key, w_value,
                               x.reshape(tiles), dout.reshape(tiles), gain)
    return (out.reshape(1, seq_len, d_model), dx.reshape(1, seq_len, d_model), gg.reshape(d_model), grad_w_query, gk, gv, grad_w_out)


def solution(mesh):
    act_spec = P('dp', None, None)

    return jax.shard_map(
        block_fn, mesh=mesh,
        in_specs=(act_spec, act_spec, P(None), P(None, 'tp'), P(None, None), P(None, None), P('tp', None)),
        out_specs=(act_spec, act_spec, P('dp'), P('dp', 'tp'), P('dp', 'tp'), P('dp', 'tp'), P(('dp', 'tp'), None)),
        check_vma=False)
```
